16 devices in a mesh: dp: 2 (over y, z), ep: 8 (over x, core).
Axes of the slice: x: 4, y: 2, z: 1, core: 2. Of those that a mesh axis runs over, the one named last changes fastest.
The devices are a block of a 4x4x8 slice.
Arguments:
- x_tokens: bfloat16 [2048, 2048], P(('dp', 'ep')), parts along dimension 0
- dy_tokens: bfloat16 [2048, 2048], P(('dp', 'ep')), parts along dimension 0
- expert_ids: int32 [2048, 10], P(('dp', 'ep')), parts along dimension 0
- gate_vals: float32 [2048, 10], P(('dp', 'ep')), parts along dimension 0
- slot_pos: int32 [2048, 10], P(('dp', 'ep')), parts along dimension 0
- w_gate: bfloat16 [32, 2048, 512], P('ep')
- w_up: bfloat16 [32, 2048, 512], P('ep')
- w_down: bfloat16 [32, 512, 2048], P('ep')
- shared_gate: bfloat16 [2048, 512], replicated
- shared_up: bfloat16 [2048, 512], replicated
- shared_down: bfloat16 [512, 2048], replicated
Outputs:
- output 1: bfloat16 [2048, 2048], P(('dp', 'ep')), parts along dimension 0
- output 2: float32 [64, 2048, 512], P(('dp', 'ep')), parts along dimension 0
- output 3: float32 [64, 2048, 512], P(('dp', 'ep')), parts along dimension 0
- output 4: float32 [64, 512, 2048], P(('dp', 'ep')), parts along dimension 0
- output 5: float32 [16, 2048, 512], P(('dp', 'ep')), parts along dimension 0
- output 6: float32 [16, 2048, 512], P(('dp', 'ep')), parts along dimension 0
- output 7: float32 [16, 512, 2048], P(('dp', 'ep')), parts along dimension 0
There are 2 independent parts. The reference program is written for one: setup_inputs(seed, part) draws one part's arguments, and reference() takes and returns one part's arrays. A program takes and returns all parts, laid end to end along the dimension named above; an argument that names none is the same for every part.
All inputs are finite; a program needn't handle non-finite values.
Results may differ from the reference program's by a relative error of at most 0.0104866.
Values are sent between devices in bfloat16 or wider.
A program may use at most 768 MiB of HBM per device.

```python
import jax
import jax.numpy as jnp
from jax import lax

MODEL_DIM = 2048
EXPERT_FF = 512
SHARED_FF = 512
TOP_K = 10
TOK_DEV = 128
GROUP_SIZE = 8
NUM_EXPERTS = 32
CAPACITY = 60


def draw_routing(route_key):
    bias_key, hot_key, noise_key = jax.random.split(route_key, 3)
    expert_range = jnp.arange(NUM_EXPERTS, dtype=jnp.int32)
    expert_bias = jax.random.randint(bias_key, (NUM_EXPERTS,), 0, 256)
    hot_expert = jax.random.randint(hot_key, (GROUP_SIZE,), 0, NUM_EXPERTS)
    noise = jax.random.randint(noise_key, (GROUP_SIZE, TOK_DEV, NUM_EXPERTS), 0, 1024)
    forced = (jnp.arange(TOK_DEV)[None, :, None] < CAPACITY) & (expert_range[None, None, :] == hot_expert[:, None, None])
    score = (noise + expert_bias[None, None, :] + 4096 * forced.astype(jnp.int32)) * NUM_EXPERTS + expert_range
    choices = lax.top_k(score, TOP_K)[1]

    def source_slots(source_choices):
        flat_choices = source_choices.reshape(-1)
        onehot = (flat_choices[:, None] == expert_range[None, :]).astype(jnp.int32)
        earlier = jnp.cumsum(onehot, axis=0) - onehot
        slot_rank = jnp.sum(earlier * onehot, axis=1)
        return jnp.where(slot_rank < CAPACITY, slot_rank, -1).reshape(TOK_DEV, TOP_K)

    positions = lax.map(source_slots, choices)
    return choices.reshape(-1, TOP_K).astype(jnp.int32), positions.reshape(-1, TOP_K).astype(jnp.int32)


def setup_inputs(seed: int = 0, part: int = 0) -> dict:
    part_key = jax.random.fold_in(jax.random.key(seed), part)
    key_x, key_dy, key_gate, key_route = jax.random.split(part_key, 4)
    weight_keys = jax.random.split(jax.random.key(seed + 1), 6)
    tokens = GROUP_SIZE * TOK_DEV
    x_tokens = jax.random.normal(key_x, (tokens, MODEL_DIM), jnp.float32).astype(jnp.bfloat16)
    dy_tokens = jax.random.normal(key_dy, (tokens, MODEL_DIM), jnp.float32).astype(jnp.bfloat16)
    gate_vals = jax.random.uniform(key_gate, (tokens, TOP_K), jnp.float32, 0.25, 1.0)
    expert_ids, slot_pos = draw_routing(key_route)
    in_scale = MODEL_DIM ** -0.5
    ff_scale = EXPERT_FF ** -0.5
    shared_scale = SHARED_FF ** -0.5
    w_gate = (jax.random.normal(weight_keys[0], (NUM_EXPERTS, MODEL_DIM, EXPERT_FF), jnp.float32) * in_scale).astype(jnp.bfloat16)
    w_up = (jax.random.normal(weight_keys[1], (NUM_EXPERTS, MODEL_DIM, EXPERT_FF), jnp.float32) * in_scale).astype(jnp.bfloat16)
    w_down = (jax.random.normal(weight_keys[2], (NUM_EXPERTS, EXPERT_FF, MODEL_DIM), jnp.float32) * ff_scale).astype(jnp.bfloat16)
    shared_gate = (jax.random.normal(weight_keys[3], (MODEL_DIM, SHARED_FF), jnp.float32) * in_scale).astype(jnp.bfloat16)
    shared_up = (jax.random.normal(weight_keys[4], (MODEL_DIM, SHARED_FF), jnp.float32) * in_scale).astype(jnp.bfloat16)
    shared_down = (jax.random.normal(weight_keys[5], (SHARED_FF, MODEL_DIM), jnp.float32) * shared_scale).astype(jnp.bfloat16)
    return {'x_tokens': x_tokens, 'dy_tokens': dy_tokens, 'expert_ids': expert_ids, 'gate_vals': gate_vals, 'slot_pos': slot_pos, 'w_gate': w_gate, 'w_up': w_up, 'w_down': w_down, 'shared_gate': shared_gate, 'shared_up': shared_up, 'shared_down': shared_down}


def expert_grads(x_rows, dz_rows, gate_w, up_w, down_w):
    act_gate = jnp.dot(x_rows, gate_w, preferred_element_type=jnp.float32).astype(jnp.bfloat16)
    act_up = jnp.dot(x_rows, up_w, preferred_element_type=jnp.float32).astype(jnp.bfloat16)
    gate_f32 = act_gate.astype(jnp.float32)
    up_f32 = act_up.astype(jnp.float32)
    sigma = jax.nn.sigmoid(gate_f32)
    silu_gate = gate_f32 * sigma
    hidden = (silu_gate * up_f32).astype(jnp.bfloat16)
    grad_hidden = jnp.dot(dz_rows, down_w.T, preferred_element_type=jnp.float32)
    grad_gate = (grad_hidden * up_f32 * sigma * (1.0 + gate_f32 * (1.0 - sigma))).astype(jnp.bfloat16)
    grad_up = (grad_hidden * silu_gate).astype(jnp.bfloat16)
    grad_down_w = jnp.dot(hidden.T, dz_rows, preferred_element_type=jnp.float32)
    grad_gate_w = jnp.dot(x_rows.T, grad_gate, preferred_element_type=jnp.float32)
    grad_up_w = jnp.dot(x_rows.T, grad_up, preferred_element_type=jnp.float32)
    grad_rows = jnp.dot(grad_gate, gate_w.T, preferred_element_type=jnp.float32) + jnp.dot(grad_up, up_w.T, preferred_element_type=jnp.float32)
    return grad_rows, grad_gate_w, grad_up_w, grad_down_w


def reference(x_tokens, dy_tokens, expert_ids, gate_vals, slot_pos, w_gate, w_up, w_down, shared_gate, shared_up, shared_down):
    tokens = GROUP_SIZE * TOK_DEV
    slot_rows = GROUP_SIZE * CAPACITY
    total_rows = NUM_EXPERTS * slot_rows
    source = jnp.arange(tokens, dtype=jnp.int32)[:, None] // TOK_DEV
    target = jnp.where(slot_pos >= 0, expert_ids * slot_rows + source * CAPACITY + slot_pos, total_rows).reshape(-1)
    token_index = jnp.broadcast_to(jnp.arange(tokens, dtype=jnp.int32)[:, None], (tokens, TOP_K)).reshape(-1)
    row_token = jnp.full((total_rows + 1,), tokens, jnp.int32).at[target].set(token_index)[:total_rows].reshape(NUM_EXPERTS, slot_rows)
    row_gate = jnp.zeros((total_rows + 1,), jnp.float32).at[target].set(gate_vals.reshape(-1))[:total_rows].reshape(NUM_EXPERTS, slot_rows)

    def expert_step(routed_sum, expert_in):
        token_rows, gate_rows, gate_w, up_w, down_w = expert_in
        x_rows = jnp.take(x_tokens, token_rows, axis=0, mode='fill', fill_value=0)
        dy_rows = jnp.take(dy_tokens, token_rows, axis=0, mode='fill', fill_value=0)
        dz_rows = (dy_rows.astype(jnp.float32) * gate_rows[:, None]).astype(jnp.bfloat16)
        grad_rows, grad_gate_w, grad_up_w, grad_down_w = expert_grads(x_rows, dz_rows, gate_w, up_w, down_w)
        returned = grad_rows.astype(jnp.bfloat16).astype(jnp.float32)
        routed_sum = routed_sum.at[token_rows].add(returned, mode='drop')
        return routed_sum, (grad_gate_w, grad_up_w, grad_down_w)

    routed_sum, expert_w_grads = lax.scan(expert_step, jnp.zeros((tokens, MODEL_DIM), jnp.float32), (row_token, row_gate, w_gate, w_up, w_down))
    grad_w_gate, grad_w_up, grad_w_down = expert_w_grads

    def shared_step(source_in):
        x_rows, dy_rows = source_in
        return expert_grads(x_rows, dy_rows, shared_gate, shared_up, shared_down)

    shared_dx, grad_shared_gate, grad_shared_up, grad_shared_down = lax.map(shared_step, (x_tokens.reshape(GROUP_SIZE, TOK_DEV, MODEL_DIM), dy_tokens.reshape(GROUP_SIZE, TOK_DEV, MODEL_DIM)))
    grad_x = (routed_sum + shared_dx.reshape(tokens, MODEL_DIM)).astype(jnp.bfloat16)
    return (grad_x, grad_w_gate, grad_w_up, grad_w_down, grad_shared_gate, grad_shared_up, grad_shared_down)
```

```python
import functools

import jax
import jax.numpy as jnp
from jax import lax
from jax.experimental import pallas as pl
from jax.experimental.pallas import tpu as pltpu
from jax.sharding import PartitionSpec as P

BF16 = jnp.bfloat16
F32 = jnp.float32
NN = (((1,), (0,)), ((), ()))
NT = (((1,), (1,)), ((), ()))
TN = (((0,), (0,)), ((), ()))
ANY = pl.BlockSpec(memory_space=pl.ANY)
VMEM = pl.BlockSpec(memory_space=pltpu.VMEM)
SMEM = pl.BlockSpec(memory_space=pltpu.SMEM)


def dot(a, b, dims=NN):
    return lax.dot_general(a, b, dims, preferred_element_type=F32)


def swiglu_parts(act_gate, act_up, grad_hidden):
    gate_f32 = act_gate.astype(BF16).astype(F32)
    up_f32 = act_up.astype(BF16).astype(F32)
    sigma = jax.nn.sigmoid(gate_f32)
    silu_gate = gate_f32 * sigma
    hidden = (silu_gate * up_f32).astype(BF16)
    grad_gate = (grad_hidden * up_f32 * sigma * (1.0 + gate_f32 * (1.0 - sigma))).astype(BF16)
    grad_up = (grad_hidden * silu_gate).astype(BF16)
    return hidden, grad_gate, grad_up


def shared_kernel(pay, wg, wu, wd, dx_t, gg, gu, gd):
    tok = pay.shape[0] // 2
    x, dy = pay[:tok, :], pay[tok:, :]
    act_gate = dot(x, wg[...])
    act_up = dot(x, wu[...])
    grad_hidden = dot(wd[...], dy, NT).T
    hidden, grad_gate, grad_up = swiglu_parts(act_gate, act_up, grad_hidden)
    hidden_t = hidden.T
    dim = wg.shape[0]
    step = 256

    @pl.loop(0, dim // step)
    def _(i):
        cols = pl.ds(pl.multiple_of(i * step, step), step)
        dx_t[cols, :] = dot(wg[cols, :], grad_gate, NT) + dot(wu[cols, :], grad_up, NT)
        x_t = pay[:tok, cols].T
        gg[0, cols, :] = dot(x_t, grad_gate)
        gu[0, cols, :] = dot(x_t, grad_up)
        gd[0, :, cols] = dot(hidden_t, pay[tok:, cols])


def shared_backward(pay, wg, wu, wd):
    dim, ff = wg.shape
    tok = pay.shape[0] // 2
    return pl.pallas_call(
        shared_kernel,
        name='shared_expert',
        out_shape=(jax.ShapeDtypeStruct((dim, tok), F32), jax.ShapeDtypeStruct((1, dim, ff), F32), jax.ShapeDtypeStruct((1, dim, ff), F32), jax.ShapeDtypeStruct((1, ff, dim), F32)),
        in_specs=[VMEM] * 4,
        out_specs=(VMEM,) * 4,
        compiler_params=pltpu.CompilerParams(vmem_limit_bytes=48 * 2**20),
        cost_estimate=pl.CostEstimate(flops=16 * tok * dim * ff, bytes_accessed=3 * dim * ff * 6, transcendentals=tok * ff),
    )(pay, wg, wu, wd)


def pass_kernel(ns, slots, top_k, *refs):
    (src, meta), pays, (w1, w3, w2) = refs[:2], refs[2:2 + ns], refs[2 + ns:5 + ns]
    x_out, z_out, d_out, h_out, p_out = refs[5 + ns:10 + ns]
    w1b, w3b, w2b, xb, zb, rb, db, hb, pb, mb, gb, wsem, xsem, dsem, psem = refs[10 + ns:]
    pairs = ns // 2
    experts, dim, ff = w1.shape
    tok = pays[0].shape[0] // 2
    pr = 2 * slots
    ebase = src[ns]
    col = 256

    def weights(e, slot):
        return [pltpu.make_async_copy(w.at[e], b.at[slot], wsem.at[slot, i]) for i, (w, b) in enumerate(((w1, w1b), (w3, w3b), (w2, w2b)))]

    for c in weights(0, 0):
        c.start()
    for p in range(pairs):
        mb[p] = jnp.zeros(mb.shape[1:], BF16)
        for s in range(2):
            info = meta[src[2 * p + s]]
            row = lax.broadcasted_iota(jnp.int32, (experts * slots, tok), 0)
            key = (row + ebase * slots).astype(F32)
            hit = jnp.zeros((experts * slots, tok), F32)
            gate = jnp.zeros((experts * slots, tok), F32)
            for j in range(top_k):
                eq = key == info[j:j + 1, :]
                hit = jnp.where(eq, 1.0, hit)
                gate = jnp.where(eq, info[16 + j:17 + j, :], gate)
            hit = hit.astype(BF16)
            gate = jnp.broadcast_to(jnp.sum(gate, axis=1, keepdims=True), (experts * slots, tok))
            for e in range(experts):
                dst = slice(e * pr + s * slots, e * pr + (s + 1) * slots)
                mb[p, dst, s * tok:(s + 1) * tok] = hit[e * slots:(e + 1) * slots]
                gb[p, dst, :] = gate[e * slots:(e + 1) * slots]

        @pl.loop(0, dim // col)
        def _(i):
            cols = pl.ds(pl.multiple_of(i * col, col), col)
            pick = mb[p]
            a, b = pays[2 * p], pays[2 * p + 1]
            xr = dot(pick, jnp.concatenate([a[:tok, cols], b[:tok, cols]], axis=0)).astype(BF16)
            yr = dot(pick, jnp.concatenate([a[tok:, cols], b[tok:, cols]], axis=0))
            g = gb[p]
            zr = (yr * jnp.concatenate([g] * (col // tok), axis=1)).astype(BF16)
            for e in range(experts):
                xb[e, p * pr:(p + 1) * pr, cols] = xr[e * pr:(e + 1) * pr]
                zb[e, p * pr:(p + 1) * pr, cols] = zr[e * pr:(e + 1) * pr]

    stash = [pltpu.make_async_copy(xb, x_out, xsem.at[0]), pltpu.make_async_copy(zb, z_out, xsem.at[1])]
    for c in stash:
        c.start()

    @pl.loop(0, experts)
    def _(e):
        slot = lax.rem(e, 2)

        @pl.when(e + 1 < experts)
        def _():
            for c in weights(e + 1, 1 - slot):
                c.start()
        for c in weights(e, slot):
            c.wait()
        act_gate = dot(xb[e], w1b[slot])
        act_up = dot(xb[e], w3b[slot])
        grad_hidden = dot(w2b[slot], zb[e], NT).T
        hidden, grad_gate, grad_up = swiglu_parts(act_gate, act_up, grad_hidden)
        db[e, :, :ff] = grad_gate
        db[e, :, ff:] = grad_up
        hb[e] = hidden.T
        pltpu.make_async_copy(db.at[e], d_out.at[e], dsem.at[0, e]).start()
        pltpu.make_async_copy(hb.at[e], h_out.at[e], dsem.at[1, e]).start()
        blk = 512

        @pl.loop(0, dim // blk)
        def _(i):
            rows = pl.ds(pl.multiple_of(i * blk, blk), blk)
            r = (dot(w1b[slot, rows, :], db[e, :, :ff], NT) + dot(w3b[slot, rows, :], db[e, :, ff:], NT)).astype(BF16)
            for p in range(pairs):
                rb[p, rows, pl.ds(pl.multiple_of(e * pr, 128), pr)] = r[:, p * pr:(p + 1) * pr]

    outs = []
    for p in range(pairs):
        blk = 512

        @pl.loop(0, dim // blk)
        def _(i):
            rows = pl.ds(pl.multiple_of(i * blk, blk), blk)
            s = dot(rb[p, rows, :], mb[p])
            pb[2 * p, rows, :] = s[:, :tok]
            pb[2 * p + 1, rows, :] = s[:, tok:]
        for s in range(2):
            c = pltpu.make_async_copy(pb.at[2 * p + s], p_out.at[s, p], psem.at[2 * p + s])
            c.start()
            outs.append(c)
    for c in outs + stash:
        c.wait()
    for e in range(experts):
        pltpu.make_async_copy(db.at[e], d_out.at[e], dsem.at[0, e]).wait()
        pltpu.make_async_copy(hb.at[e], h_out.at[e], dsem.at[1, e]).wait()


def expert_pass(name, src, meta, pays, w1, w3, w2, slots, top_k):
    experts, dim, ff = w1.shape
    ns = len(pays)
    tok = pays[0].shape[0] // 2
    rows = ns * slots
    pairs = ns // 2
    flops = 2 * experts * rows * dim * ff * 5 + 4 * 2 * experts * rows * 256 * dim
    return pl.pallas_call(
        functools.partial(pass_kernel, ns, slots, top_k),
        name=name,
        out_shape=(jax.ShapeDtypeStruct((experts, rows, dim), BF16), jax.ShapeDtypeStruct((experts, rows, dim), BF16), jax.ShapeDtypeStruct((experts, rows, 2 * ff), BF16), jax.ShapeDtypeStruct((experts, ff, rows), BF16), jax.ShapeDtypeStruct((2, pairs, dim, tok), F32)),
        in_specs=[SMEM, VMEM] + [VMEM] * ns + [ANY] * 3,
        out_specs=(ANY,) * 5,
        scratch_shapes=[
            pltpu.VMEM((2, dim, ff), BF16), pltpu.VMEM((2, dim, ff), BF16), pltpu.VMEM((2, ff, dim), BF16),
            pltpu.VMEM((experts, rows, dim), BF16), pltpu.VMEM((experts, rows, dim), BF16),
            pltpu.VMEM((pairs, dim, experts * 2 * slots), BF16),
            pltpu.VMEM((experts, rows, 2 * ff), BF16), pltpu.VMEM((experts, ff, rows), BF16),
            pltpu.VMEM((ns, dim, tok), F32),
            pltpu.VMEM((pairs, experts * 2 * slots, 2 * tok), BF16), pltpu.VMEM((pairs, experts * 2 * slots, tok), F32),
            pltpu.SemaphoreType.DMA((2, 3)), pltpu.SemaphoreType.DMA((2,)), pltpu.SemaphoreType.DMA((2, experts)), pltpu.SemaphoreType.DMA((ns,)),
        ],
        compiler_params=pltpu.CompilerParams(vmem_limit_bytes=56 * 2**20),
        cost_estimate=pl.CostEstimate(flops=flops, bytes_accessed=3 * experts * dim * ff * 2 + experts * rows * dim * 4 + ns * tok * dim * 8, transcendentals=experts * rows * ff),
    )(src, meta, *pays, w1, w3, w2)


def grad_kernel(n, *refs):
    xs, zs, ds, hs = refs[:n], refs[n:2 * n], refs[2 * n:3 * n], refs[3 * n:4 * n]
    g1, g3, g2 = refs[4 * n:]
    ff = g1.shape[2]
    x = jnp.concatenate([r[0] for r in xs], axis=0)
    z = jnp.concatenate([r[0] for r in zs], axis=0)
    d = jnp.concatenate([r[0] for r in ds], axis=0)
    h = jnp.concatenate([r[0] for r in hs], axis=1)
    x_t = x.T
    g1[0] = dot(x_t, d[:, :ff])
    g3[0] = dot(x_t, d[:, ff:])
    g2[0] = dot(h, z)


def weight_grads(parts, ff):
    xs, zs, ds, hs = zip(*parts)
    n = len(parts)
    experts, _, dim = xs[0].shape
    blk = 512

    def rows_spec(a):
        return pl.BlockSpec((1, a.shape[1], blk), lambda e, i: (e, 0, i))

    def whole_spec(a):
        return pl.BlockSpec((1,) + a.shape[1:], lambda e, i: (e, 0, 0))

    total = sum(a.shape[1] for a in xs)
    return pl.pallas_call(
        functools.partial(grad_kernel, n),
        name='weight_grads',
        grid=(experts, dim // blk),
        in_specs=[rows_spec(a) for a in xs + zs] + [whole_spec(a) for a in ds + hs],
        out_specs=(pl.BlockSpec((1, blk, ff), lambda e, i: (e, i, 0)), pl.BlockSpec((1, blk, ff), lambda e, i: (e, i, 0)), pl.BlockSpec((1, ff, blk), lambda e, i: (e, 0, i))),
        out_shape=(jax.ShapeDtypeStruct((experts, dim, ff), F32), jax.ShapeDtypeStruct((experts, dim, ff), F32), jax.ShapeDtypeStruct((experts, ff, dim), F32)),
        compiler_params=pltpu.CompilerParams(vmem_limit_bytes=40 * 2**20),
        cost_estimate=pl.CostEstimate(flops=6 * experts * total * dim * ff, bytes_accessed=experts * dim * (total * 4 + ff * 12), transcendentals=0),
    )(*xs, *zs, *ds, *hs)


def final_kernel(a, b, c, d, out):
    out[...] = (((a[...] + b[...]) + c[...]) + d[...]).T.astype(BF16)


def final_sum(*terms):
    dim, tok = terms[0].shape
    blk = 512
    return pl.pallas_call(
        final_kernel,
        name='final_sum',
        grid=(dim // blk,),
        in_specs=[pl.BlockSpec((blk, tok), lambda i: (i, 0))] * 4,
        out_specs=pl.BlockSpec((tok, blk), lambda i: (0, i)),
        out_shape=jax.ShapeDtypeStruct((tok, dim), BF16),
        cost_estimate=pl.CostEstimate(flops=5 * dim * tok, bytes_accessed=dim * tok * 22, transcendentals=0),
    )(*terms)


def solution(mesh):
    group = mesh.shape['ep']
    cores = 2
    chips = group // cores
    token_spec = P(('dp', 'ep'), None)
    expert_spec = P('ep', None, None)
    whole_spec = P(None, None)
    grad_spec = P(('dp', 'ep'), None, None)

    def dev(chip, core):
        return (chip % chips) * cores + core

    def shift(step):
        return [(dev(c, k), dev(c + (step if k == 0 else -step), k)) for c in range(chips) for k in range(cores)]

    partner = [(d, d ^ 1) for d in range(group)]

    def send(v, perm):
        return lax.ppermute(v, 'ep', perm)

    def local_backward(x_tokens, dy_tokens, expert_ids, gate_vals, slot_pos, w_gate, w_up, w_down, shared_gate, shared_up, shared_down):
        tok, top_k = expert_ids.shape
        local_experts, dim, ff = w_gate.shape
        num_experts = local_experts * group
        capacity = (3 * tok * top_k + 2 * num_experts - 1) // (2 * num_experts)
        slots = pl.cdiv(capacity, 64) * 64
        me = lax.axis_index('ep')
        chip, core = me // cores, lax.rem(me, cores)
        sign = 1 - 2 * core

        def source(step, other):
            k = core if not other else 1 - core
            s = sign if not other else -sign
            return lax.rem(chip - s * step + 2 * chips, chips) * cores + k

        pay = jnp.concatenate([x_tokens, dy_tokens], axis=0)
        key = jnp.where(slot_pos >= 0, expert_ids * slots + slot_pos, -1).astype(F32).T
        key = jnp.pad(key, ((0, 16 - top_k), (0, 0)), constant_values=-1.0)
        gates = jnp.pad(gate_vals.T, ((0, 16 - top_k), (0, 0)))
        meta = lax.all_gather(jnp.concatenate([key, gates], axis=0), 'ep')

        near = send(pay, shift(1))
        pay_other = send(pay, partner)
        near_other = send(near, partner)
        far = send(near, shift(1))
        back_in, _ = lax.optimization_barrier((pay, near))
        back = send(back_in, shift(-1))
        far_other = send(far, partner)
        back_other = send(back, partner)
        shared_dx, gsg, gsu, gsd = shared_backward(pay, shared_gate, shared_up, shared_down)

        ebase = me * local_experts
        src1 = jnp.stack([source(0, False), source(0, True), source(1, False), source(1, True), ebase]).astype(jnp.int32)
        src2 = jnp.stack([source(2, False), source(2, True), source(-1, False), source(-1, True), ebase]).astype(jnp.int32)
        x1, z1, d1, h1, p1 = expert_pass('pass_near', src1, meta, (pay, pay_other, near, near_other), w_gate, w_up, w_down, slots, top_k)
        got1 = send(p1[1], partner)
        own_sum = p1[0, 0] + got1[0]
        near_sum = p1[0, 1] + got1[1]
        ret_near = send(near_sum, shift(-1))
        x2, z2, d2, h2, p2 = expert_pass('pass_far', src2, meta, (far, far_other, back, back_other), w_gate, w_up, w_down, slots, top_k)
        got2 = send(p2[1], partner)
        far_sum = p2[0, 0] + got2[0]
        via = send(far_sum, shift(1))
        back_sum = p2[0, 1] + got2[1] + via
        ret_back = send(back_sum, shift(1))
        g1, g3, g2 = weight_grads(((x1, z1, d1, h1), (x2, z2, d2, h2)), ff)
        grad_x = final_sum(shared_dx, own_sum, ret_near, ret_back)
        return grad_x, g1, g3, g2, gsg, gsu, gsd

    return jax.shard_map(local_backward, mesh=mesh, in_specs=(token_spec, token_spec, token_spec, token_spec, token_spec, expert_spec, expert_spec, expert_spec, whole_spec, whole_spec, whole_spec), out_specs=(token_spec, grad_spec, grad_spec, grad_spec, grad_spec, grad_spec, grad_spec), check_vma=False)
```

```python
import functools

import jax
import jax.numpy as jnp
from jax import lax
from jax.experimental import pallas as pl
from jax.experimental.pallas import tpu as pltpu
from jax.sharding import PartitionSpec as P

BF16 = jnp.bfloat16
F32 = jnp.float32
NN = (((1,), (0,)), ((), ()))
NT = (((1,), (1,)), ((), ()))
TN = (((0,), (0,)), ((), ()))
ANY = pl.BlockSpec(memory_space=pl.ANY)
VMEM = pl.BlockSpec(memory_space=pltpu.VMEM)
SMEM = pl.BlockSpec(memory_space=pltpu.SMEM)


def dot(a, b, dims=NN):
    return lax.dot_general(a, b, dims, preferred_element_type=F32)


def swiglu_parts(act_gate, act_up, grad_hidden):
    gate_f32 = act_gate.astype(BF16).astype(F32)
    up_f32 = act_up.astype(BF16).astype(F32)
    sigma = jax.nn.sigmoid(gate_f32)
    silu_gate = gate_f32 * sigma
    hidden = (silu_gate * up_f32).astype(BF16)
    grad_gate = (grad_hidden * up_f32 * sigma * (1.0 + gate_f32 * (1.0 - sigma))).astype(BF16)
    grad_up = (grad_hidden * silu_gate).astype(BF16)
    return hidden, grad_gate, grad_up


def layer_kernel(chips, top_k, slots, x, dy, ids, pos, gates, w1, w3, w2, sg, su, sd,
                 x_out, z_out, d_out, h_out, ds_out, hs_out, own_out, near_out, back_out,
                 xg, yg, meta, keys, w1b, w3b, w2b, xb, zb, rb, db, hb, dsb, hsb, shr, pb, pr, via, mb, gb,
                 lsem, wsem, osem, msend, mrecv, xsend, xrecv, ysend, yrecv, psend, precv, vsem):
    experts, dim, ff = w1.shape
    tok = x.shape[0]
    pairw = 2 * slots
    me = lax.axis_index('ep')
    core = lax.rem(me, 2)
    chip = me // 2
    sign = 1 - 2 * core

    def device(step, other):
        return lax.rem(chip + sign * step + chips, chips) * 2 + (1 - core if other else core)

    partner, nxt, prv = device(0, True), device(1, False), device(-1, False)
    peers = [(partner, 1), (nxt, 2), (device(1, True), 3), (device(2, False), 4), (device(2, True), 5), (prv, 6), (device(-1, True), 7)]

    def remote(src, dst, ss, rs, to):
        return pltpu.make_async_remote_copy(src_ref=src, dst_ref=dst, send_sem=ss, recv_sem=rs, device_id={'ep': to}, device_id_type=pl.DeviceIdType.MESH)

    def tokens(frm, to_slot, to):
        return [remote(xg.at[frm], xg.at[to_slot], xsend.at[to_slot], xrecv.at[to_slot], to),
                remote(yg.at[frm], yg.at[to_slot], ysend.at[to_slot], yrecv.at[to_slot], to)]

    def start(copies):
        for c in copies:
            c.start()

    own = [pltpu.make_async_copy(x, xg.at[0], lsem.at[0]), pltpu.make_async_copy(dy, yg.at[0], lsem.at[1])]
    start(own)
    barrier = pltpu.get_barrier_semaphore()
    for to, _ in peers:
        pl.semaphore_signal(barrier, inc=1, device_id={'ep': to}, device_id_type=pl.DeviceIdType.MESH)
    pl.semaphore_wait(barrier, len(peers))

    to_next, to_partner, to_prev = tokens(0, 2, nxt), tokens(0, 1, partner), tokens(0, 6, prv)
    near_on, near_side, far_side, back_side = tokens(2, 4, nxt), tokens(2, 3, partner), tokens(4, 5, partner), tokens(6, 7, partner)
    for c in own:
        c.wait()
    start(to_next)
    start(to_partner)

    def loads(srcs, slot):
        return [pltpu.make_async_copy(w, b.at[slot], wsem.at[i, slot]) for i, (w, b) in enumerate(zip(srcs, (w1b, w3b, w2b)))]

    last = experts - 1
    shared_load = [pltpu.make_async_copy(w, b.at[last], wsem.at[i, experts]) for i, (w, b) in enumerate(zip((sg, su, sd), (w1b, w3b, w2b)))]
    start(shared_load)
    expert_loads = [loads((w1.at[e], w3.at[e], w2.at[e]), e) for e in range(experts)]
    for e in range(last):
        start(expert_loads[e])

    keys[0, :, :top_k] = jnp.where(pos[...] >= 0, ids[...] * slots + pos[...], -1).astype(F32)
    keys[1, :, :top_k] = gates[...]
    meta[0, :16] = keys[0].T[:16]
    meta[0, 16:] = keys[1].T[:16]
    metas = [remote(meta.at[0], meta.at[s], msend.at[s], mrecv.at[s], to) for to, s in peers]
    start(metas)

    for c in shared_load:
        c.wait()
    act_gate = dot(xg[0], w1b[last])
    act_up = dot(xg[0], w3b[last])
    hidden, grad_gate, grad_up = swiglu_parts(act_gate, act_up, dot(w2b[last], yg[0], NT).T)
    dsb[:, :ff] = grad_gate
    dsb[:, ff:] = grad_up
    hsb[...] = hidden.T
    shared_out = [pltpu.make_async_copy(dsb, ds_out, osem.at[0]), pltpu.make_async_copy(hsb, hs_out, osem.at[1])]
    start(shared_out)
    blk = 512

    def block(i):
        return pl.ds(pl.multiple_of(i * blk, blk), blk)

    @pl.loop(0, dim // blk)
    def _(i):
        shr[block(i), :] = dot(w1b[last, block(i), :], dsb[:, :ff], NT) + dot(w3b[last, block(i), :], dsb[:, ff:], NT)

    start(expert_loads[last])

    def pick(p, a, b):
        mb[p] = jnp.zeros(mb.shape[1:], BF16)
        for s, slot in enumerate((a, b)):
            info = meta[slot]
            row = lax.broadcasted_iota(jnp.int32, (experts * slots, tok), 0)
            key = (row + me * (experts * slots)).astype(F32)
            hit = jnp.zeros((experts * slots, tok), F32)
            gate = jnp.zeros((experts * slots, tok), F32)
            for j in range(top_k):
                eq = key == info[j:j + 1, :]
                hit = jnp.where(eq, 1.0, hit)
                gate = jnp.where(eq, info[16 + j:17 + j, :], gate)
            hit = hit.astype(BF16)
            gate = jnp.broadcast_to(jnp.sum(gate, axis=1, keepdims=True), (experts * slots, tok))
            for e in range(experts):
                dst = slice(e * pairw + s * slots, e * pairw + (s + 1) * slots)
                mb[p, dst, s * tok:(s + 1) * tok] = hit[e * slots:(e + 1) * slots]
                gb[p, dst, :] = gate[e * slots:(e + 1) * slots]
        col = 256

        @pl.loop(0, dim // col)
        def _(i):
            cols = pl.ds(pl.multiple_of(i * col, col), col)
            xr = dot(mb[p], jnp.concatenate([xg[a, :, cols], xg[b, :, cols]], axis=0)).astype(BF16)
            for e in range(experts):
                xb[e, p * pairw:(p + 1) * pairw, cols] = xr[e * pairw:(e + 1) * pairw]
            zr = dot(mb[p], jnp.concatenate([yg[a, :, cols], yg[b, :, cols]], axis=0))
            zr = (zr * jnp.concatenate([gb[p]] * (col // tok), axis=1)).astype(BF16)
            for e in range(experts):
                zb[e, p * pairw:(p + 1) * pairw, cols] = zr[e * pairw:(e + 1) * pairw]

    def keep(first, rows, n):
        return [pltpu.make_async_copy(xb.at[:, :rows], x_out.at[:, first:first + rows], osem.at[n]),
                pltpu.make_async_copy(zb.at[:, :rows], z_out.at[:, first:first + rows], osem.at[n + 1]),
                pltpu.make_async_copy(db.at[:, :rows], d_out.at[:, first:first + rows], osem.at[n + 2]),
                pltpu.make_async_copy(hb.at[:, :, :rows], h_out.at[:, :, first:first + rows], osem.at[n + 3])]

    def run_experts(rows, events):
        @pl.loop(0, experts)
        def _(e):
            for at, event in events:
                pl.when(e == at)(event)
            xe = xb[e, :rows, :]
            act_gate = dot(xe, w1b[e])
            act_up = dot(xe, w3b[e])
            grad_hidden = dot(w2b[e], zb[e, :rows, :], NT).T
            hidden, grad_gate, grad_up = swiglu_parts(act_gate, act_up, grad_hidden)
            db[e, :rows, :ff] = grad_gate
            db[e, :rows, ff:] = grad_up
            hb[e, :, :rows] = hidden.T

            @pl.loop(0, dim // blk)
            def _(i):
                r = (dot(w1b[e, block(i), :], db[e, :rows, :ff], NT) + dot(w3b[e, block(i), :], db[e, :rows, ff:], NT)).astype(BF16)
                for p in range(rows // pairw):
                    rb[p, block(i), pl.ds(pl.multiple_of(e * pairw, pairw), pairw)] = r[:, p * pairw:(p + 1) * pairw]

    def combine(p, first):
        @pl.loop(0, dim // blk)
        def _(i):
            s = dot(rb[p, block(i), :], mb[p])
            pb[first, block(i), :] = s[:, :tok]
            pb[first + 1, block(i), :] = s[:, tok:]

    def wait_recv(copies):
        for c in copies:
            c.wait_recv()

    def side(frm, to_slot):
        return remote(pb.at[frm], pr.at[to_slot], psend.at[to_slot], precv.at[to_slot], partner)

    def add(to_slot, terms):
        @pl.loop(0, dim // blk)
        def _(i):
            v = pr[to_slot, block(i), :]
            for t in terms:
                v = v + t[block(i), :]
            pr[to_slot, block(i), :] = v

    wait_recv(metas)
    wait_recv(to_partner)
    pick(0, 0, 1)
    wait_recv(to_next)
    start(near_on)
    start(near_side)
    wait_recv(near_side)
    pick(1, 2, 3)
    keep_a = keep(0, 2 * pairw, 2)
    start(keep_a[:2])

    for c in expert_loads[0]:
        c.wait()

    def more_weights(e):
        def event():
            for c in expert_loads[e]:
                c.wait()
        return event

    def send_back():
        wait_recv(near_on)
        start(far_side)
        start(to_prev)

    run_experts(2 * pairw, [(e, more_weights(e)) for e in range(1, experts)] + [(last, send_back)])
    start(keep_a[2:])
    combine(0, 0)
    to_own = side(1, 0)
    to_own.start()
    combine(1, 2)
    to_near = side(3, 1)
    to_near.start()

    for c in keep_a:
        c.wait()
    wait_recv(far_side)
    pick(0, 4, 5)
    keep_b = keep(2 * pairw, pairw, 6)
    start(keep_b[:2])
    sums = [pltpu.make_async_copy(pr.at[0], own_out, osem.at[14]), pltpu.make_async_copy(pr.at[1], near_out, osem.at[15])]

    def sum_near():
        to_own.wait()
        add(0, [pb.at[0], shr])
        to_near.wait()
        add(1, [pb.at[2]])
        start(sums)

    def take_back():
        wait_recv(to_prev)
        start(back_side)

    run_experts(pairw, [(2, sum_near), (last, take_back)])
    start(keep_b[2:])
    combine(0, 0)
    to_far = side(1, 2)
    to_far.start()

    for c in keep_b:
        c.wait()
    wait_recv(back_side)
    pick(0, 6, 7)
    keep_c = keep(3 * pairw, pairw, 10)
    start(keep_c[:2])
    pass_on = remote(pr.at[2], via, vsem.at[0], vsem.at[1], nxt)

    def sum_far():
        to_far.wait()
        add(2, [pb.at[0]])
        pass_on.start()

    run_experts(pairw, [(1, sum_far)])
    start(keep_c[2:])
    combine(0, 2)
    to_back = side(3, 3)
    to_back.start()
    to_back.wait()
    pass_on.wait()
    add(3, [pb.at[2], via])
    back_copy = pltpu.make_async_copy(pr.at[3], back_out, osem.at[16])
    back_copy.start()
    for c in shared_out + keep_c + sums + [back_copy]:
        c.wait()
    for copies in (to_next, to_partner, to_prev, near_on, near_side, far_side, back_side, metas):
        for c in copies:
            c.wait_send()


def layer(chips, x, dy, ids, pos, gates, weights, shared, slots):
    experts, dim, ff = weights[0].shape
    tok, top_k = ids.shape
    pairw = 2 * slots
    rows = chips * pairw
    half = 2 * pairw
    dma = pltpu.SemaphoreType.DMA
    sds = jax.ShapeDtypeStruct
    hbm = pl.BlockSpec(memory_space=pltpu.HBM)
    return pl.pallas_call(
        functools.partial(layer_kernel, chips, top_k, slots),
        name='layer',
        out_shape=(sds((experts, rows, dim), BF16), sds((experts, rows, dim), BF16), sds((experts, rows, 2 * ff), BF16), sds((experts, ff, rows), BF16),
                   sds((tok, 2 * ff), BF16), sds((ff, tok), BF16), sds((dim, tok), F32), sds((dim, tok), F32), sds((dim, tok), F32)),
        in_specs=[hbm] * 2 + [VMEM] * 3 + [hbm] * 6,
        out_specs=(hbm,) * 9,
        scratch_shapes=[
            pltpu.VMEM((8, tok, dim), BF16), pltpu.VMEM((8, tok, dim), BF16), pltpu.VMEM((8, 32, tok), F32), pltpu.VMEM((2, tok, 128), F32),
            pltpu.VMEM((experts, dim, ff), BF16), pltpu.VMEM((experts, dim, ff), BF16), pltpu.VMEM((experts, ff, dim), BF16),
            pltpu.VMEM((experts, half, dim), BF16), pltpu.VMEM((experts, half, dim), BF16),
            pltpu.VMEM((2, dim, experts * pairw), BF16),
            pltpu.VMEM((experts, half, 2 * ff), BF16), pltpu.VMEM((experts, ff, half), BF16),
            pltpu.VMEM((tok, 2 * ff), BF16), pltpu.VMEM((ff, tok), BF16), pltpu.VMEM((dim, tok), F32),
            pltpu.VMEM((4, dim, tok), F32), pltpu.VMEM((4, dim, tok), F32), pltpu.VMEM((dim, tok), F32),
            pltpu.VMEM((2, experts * pairw, 2 * tok), BF16), pltpu.VMEM((2, experts * pairw, tok), F32),
            dma((2,)), dma((3, experts + 1)), dma((17,)), dma((8,)), dma((8,)), dma((8,)), dma((8,)), dma((8,)), dma((8,)), dma((4,)), dma((4,)), dma((2,)),
        ],
        compiler_params=pltpu.CompilerParams(vmem_limit_bytes=67043328, collective_id=0, has_side_effects=True),
        cost_estimate=pl.CostEstimate(flops=10 * experts * rows * dim * ff, bytes_accessed=3 * experts * dim * ff * 2, transcendentals=experts * rows * ff),
    )(x, dy, ids, pos, gates, *weights, *shared)


def shared_grad_kernel(x, z, d, h, g1, g3, g2):
    ff = g1.shape[2]
    x_t = x[...].T
    g1[0] = dot(x_t, d[:, :ff])
    g3[0] = dot(x_t, d[:, ff:])
    g2[0] = dot(h[...], z[...])


def shared_grads(x, z, d, h):
    tok, dim = x.shape
    ff = h.shape[0]
    blk = 512
    return pl.pallas_call(
        shared_grad_kernel,
        name='shared_grads',
        grid=(dim // blk,),
        in_specs=[pl.BlockSpec((tok, blk), lambda i: (0, i))] * 2 + [pl.BlockSpec(d.shape, lambda i: (0, 0)), pl.BlockSpec(h.shape, lambda i: (0, 0))],
        out_specs=(pl.BlockSpec((1, blk, ff), lambda i: (0, i, 0)), pl.BlockSpec((1, blk, ff), lambda i: (0, i, 0)), pl.BlockSpec((1, ff, blk), lambda i: (0, 0, i))),
        out_shape=(jax.ShapeDtypeStruct((1, dim, ff), F32), jax.ShapeDtypeStruct((1, dim, ff), F32), jax.ShapeDtypeStruct((1, ff, dim), F32)),
        cost_estimate=pl.CostEstimate(flops=6 * tok * dim * ff, bytes_accessed=12 * dim * ff, transcendentals=0),
    )(x, z, d, h)


def grad_kernel(n, *refs):
    xs, zs, ds, hs = refs[:n], refs[n:2 * n], refs[2 * n:3 * n], refs[3 * n:4 * n]
    g1, g3, g2 = refs[4 * n:]
    ff = g1.shape[2]
    x = jnp.concatenate([r[0] for r in xs], axis=0)
    z = jnp.concatenate([r[0] for r in zs], axis=0)
    d = jnp.concatenate([r[0] for r in ds], axis=0)
    h = jnp.concatenate([r[0] for r in hs], axis=1)
    x_t = x.T
    g1[0] = dot(x_t, d[:, :ff])
    g3[0] = dot(x_t, d[:, ff:])
    g2[0] = dot(h, z)


def weight_grads(parts, ff):
    xs, zs, ds, hs = zip(*parts)
    n = len(parts)
    experts, _, dim = xs[0].shape
    blk = 512

    def rows_spec(a):
        return pl.BlockSpec((1, a.shape[1], blk), lambda e, i: (e, 0, i))

    def whole_spec(a):
        return pl.BlockSpec((1,) + a.shape[1:], lambda e, i: (e, 0, 0))

    total = sum(a.shape[1] for a in xs)
    return pl.pallas_call(
        functools.partial(grad_kernel, n),
        name='weight_grads',
        grid=(experts, dim // blk),
        in_specs=[rows_spec(a) for a in xs + zs] + [whole_spec(a) for a in ds + hs],
        out_specs=(pl.BlockSpec((1, blk, ff), lambda e, i: (e, i, 0)), pl.BlockSpec((1, blk, ff), lambda e, i: (e, i, 0)), pl.BlockSpec((1, ff, blk), lambda e, i: (e, 0, i))),
        out_shape=(jax.ShapeDtypeStruct((experts, dim, ff), F32), jax.ShapeDtypeStruct((experts, dim, ff), F32), jax.ShapeDtypeStruct((experts, ff, dim), F32)),
        compiler_params=pltpu.CompilerParams(vmem_limit_bytes=40 * 2**20),
        cost_estimate=pl.CostEstimate(flops=6 * experts * total * dim * ff, bytes_accessed=experts * dim * (total * 4 + ff * 12), transcendentals=0),
    )(*xs, *zs, *ds, *hs)


def final_kernel(a, b, c, out):
    out[...] = ((a[...] + b[...]) + c[...]).T.astype(BF16)


def final_sum(*terms):
    dim, tok = terms[0].shape
    blk = 512
    return pl.pallas_call(
        final_kernel,
        name='final_sum',
        grid=(dim // blk,),
        in_specs=[pl.BlockSpec((blk, tok), lambda i: (i, 0))] * 3,
        out_specs=pl.BlockSpec((tok, blk), lambda i: (0, i)),
        out_shape=jax.ShapeDtypeStruct((tok, dim), BF16),
        cost_estimate=pl.CostEstimate(flops=5 * dim * tok, bytes_accessed=dim * tok * 22, transcendentals=0),
    )(*terms)


def solution(mesh):
    group = mesh.shape['ep']
    cores = 2
    chips = group // cores
    token_spec = P(('dp', 'ep'), None)
    expert_spec = P('ep', None, None)
    whole_spec = P(None, None)
    grad_spec = P(('dp', 'ep'), None, None)

    assert chips == 4

    def shift(step):
        return [(c * cores + k, ((c + (step if k == 0 else -step)) % chips) * cores + k) for c in range(chips) for k in range(cores)]

    def local_backward(x_tokens, dy_tokens, expert_ids, gate_vals, slot_pos, w_gate, w_up, w_down, shared_gate, shared_up, shared_down):
        tok, top_k = expert_ids.shape
        num_experts = w_gate.shape[0] * group
        ff = w_gate.shape[2]
        capacity = (3 * tok * top_k + 2 * num_experts - 1) // (2 * num_experts)
        slots = pl.cdiv(capacity, 64) * 64
        x, z, d, h, ds, hs, own_sum, near_sum, back_sum = layer(chips, x_tokens, dy_tokens, expert_ids, slot_pos, gate_vals, (w_gate, w_up, w_down), (shared_gate, shared_up, shared_down), slots)
        ret_near = lax.ppermute(near_sum, 'ep', shift(-1))
        ret_back = lax.ppermute(back_sum, 'ep', shift(1))
        g1, g3, g2 = weight_grads(((x, z, d, h),), ff)
        gsg, gsu, gsd = shared_grads(x_tokens, dy_tokens, ds, hs)
        grad_x = final_sum(own_sum, ret_near, ret_back)
        return grad_x, g1, g3, g2, gsg, gsu, gsd

    return jax.shard_map(local_backward, mesh=mesh, in_specs=(token_spec, token_spec, token_spec, token_spec, token_spec, expert_spec, expert_spec, expert_spec, whole_spec, whole_spec, whole_spec), out_specs=(token_spec, grad_spec, grad_spec, grad_spec, grad_spec, grad_spec, grad_spec), check_vma=False)
```

```python
import functools

import jax
import jax.numpy as jnp
from jax import lax
from jax.experimental import pallas as pl
from jax.experimental.pallas import tpu as pltpu
from jax.sharding import PartitionSpec as P

BF16 = jnp.bfloat16
F32 = jnp.float32
NN = (((1,), (0,)), ((), ()))
NT = (((1,), (1,)), ((), ()))
TN = (((0,), (0,)), ((), ()))
ANY = pl.BlockSpec(memory_space=pl.ANY)
VMEM = pl.BlockSpec(memory_space=pltpu.VMEM)
SMEM = pl.BlockSpec(memory_space=pltpu.SMEM)


def dot(a, b, dims=NN):
    return lax.dot_general(a, b, dims, preferred_element_type=F32)


def swiglu_parts(act_gate, act_up, grad_hidden):
    gate_f32 = act_gate.astype(F32)
    up_f32 = act_up.astype(F32)
    sigma = jax.nn.sigmoid(gate_f32)
    silu_gate = gate_f32 * sigma
    hidden = (silu_gate * up_f32).astype(BF16)
    grad_gate = (grad_hidden * up_f32 * sigma * (1.0 + gate_f32 * (1.0 - sigma))).astype(BF16)
    grad_up = (grad_hidden * silu_gate).astype(BF16)
    return hidden, grad_gate, grad_up


def layer_kernel(chips, top_k, slots, x, dy, ids, pos, gates, w1, w3, w2, sg, su, sd,
                 x_out, z_out, d_out, h_out, ds_out, hs_out, own_out, near_out, far_out, back_out,
                 xg, yg, meta, w1b, w3b, w2b, rows_b, rb, db, hb, dsb, hsb, shr, pb, pr, ret, mb, gb,
                 lsem, wsem, osem, msend, mrecv, xsend, xrecv, ysend, yrecv, psend, precv, rsem):
    experts, dim, ff = w1.shape
    tok = x.shape[0]
    pairw = 2 * slots
    half = 2 * pairw
    me = lax.axis_index('ep')
    core = lax.rem(me, 2)
    chip = me // 2
    sign = 1 - 2 * core

    def device(step, other):
        return lax.rem(chip + sign * step + chips, chips) * 2 + (1 - core if other else core)

    partner, nxt, prv = device(0, True), device(1, False), device(-1, False)
    peers = [(partner, 1), (nxt, 2), (device(1, True), 3), (device(2, False), 4), (device(2, True), 5), (prv, 6), (device(-1, True), 7)]

    def remote(src, dst, ss, rs, to):
        return pltpu.make_async_remote_copy(src_ref=src, dst_ref=dst, send_sem=ss, recv_sem=rs, device_id={'ep': to}, device_id_type=pl.DeviceIdType.MESH)

    def send_x(frm, slot, to):
        return remote(xg.at[frm], xg.at[slot], xsend.at[slot], xrecv.at[slot], to)

    def send_y(frm, slot, to):
        return remote(yg.at[frm], yg.at[slot], ysend.at[slot], yrecv.at[slot], to)

    def start(copies):
        for c in copies:
            c.start()

    own = [pltpu.make_async_copy(x, xg.at[0], lsem.at[0]), pltpu.make_async_copy(dy, yg.at[0], lsem.at[1])]
    start(own)
    barrier = pltpu.get_barrier_semaphore()
    for to, _ in peers:
        pl.semaphore_signal(barrier, inc=1, device_id={'ep': to}, device_id_type=pl.DeviceIdType.MESH)
    pl.semaphore_wait(barrier, len(peers))

    routes = ((0, 1, partner), (0, 2, nxt), (2, 3, partner), (2, 4, nxt), (4, 5, partner), (0, 6, prv), (6, 7, partner))
    xs = {slot: send_x(frm, slot, to) for frm, slot, to in routes}
    ys = {slot: send_y(frm, slot, to) for frm, slot, to in routes}
    own[0].wait()
    xs[2].start()
    xs[1].start()
    own[1].wait()
    ys[1].start()

    def loads(srcs, slot, n):
        return [pltpu.make_async_copy(w, b.at[slot], wsem.at[i, n]) for i, (w, b) in enumerate(zip(srcs, (w1b, w3b, w2b)))]

    last = experts - 1
    shared_load = loads((sg, su, sd), last, experts)
    start(shared_load)
    expert_loads = [loads((w1.at[e], w3.at[e], w2.at[e]), e, e) for e in range(experts)]
    for e in range(last):
        start(expert_loads[e])

    meta[0, :top_k] = jnp.where(pos[...] >= 0, ids[...] * slots + pos[...], -1).astype(F32)
    meta[0, 16:16 + top_k] = gates[...]
    metas = [remote(meta.at[0], meta.at[s], msend.at[s], mrecv.at[s], to) for to, s in peers]
    start(metas)
    blk = 512

    def block(i):
        return pl.ds(pl.multiple_of(i * blk, blk), blk)

    def wait_recv(copies):
        for c in copies:
            c.wait_recv()

    def pick(p, a, b):
        mb[p] = jnp.zeros(mb.shape[1:], BF16)
        for s, slot in enumerate((a, b)):
            info = meta[slot]
            row = lax.broadcasted_iota(jnp.int32, (experts * slots, tok), 0)
            key = (row + me * (experts * slots)).astype(F32)
            hit = jnp.zeros((experts * slots, tok), F32)
            gate = jnp.zeros((experts * slots, tok), F32)
            for j in range(top_k):
                eq = key == info[j:j + 1, :]
                hit = jnp.where(eq, 1.0, hit)
                gate = jnp.where(eq, info[16 + j:17 + j, :], gate)
            hit = hit.astype(BF16)
            gate = jnp.broadcast_to(jnp.sum(gate, axis=1, keepdims=True), (experts * slots, tok))
            for e in range(experts):
                dst = slice(e * pairw + s * slots, e * pairw + (s + 1) * slots)
                mb[p, dst, s * tok:(s + 1) * tok] = hit[e * slots:(e + 1) * slots]
                gb[p, dst, :] = gate[e * slots:(e + 1) * slots]

    def gather(src, p, a, b, gated):
        col = 256
        at = (p % 2) * pairw

        @pl.loop(0, dim // col)
        def _(i):
            cols = pl.ds(pl.multiple_of(i * col, col), col)
            r = dot(mb[p], jnp.concatenate([src[a, :, cols], src[b, :, cols]], axis=0))
            if gated:
                r = r * jnp.concatenate([gb[p]] * (col // tok), axis=1)
            r = r.astype(BF16)
            for e in range(experts):
                rows_b[e, at:at + pairw, cols] = r[e * pairw:(e + 1) * pairw]

    def kept(out, g, n):
        return pltpu.make_async_copy(rows_b, out.at[:, g * half:(g + 1) * half], osem.at[n])

    def expert_loop(body, events):
        @pl.loop(0, experts)
        def _(e):
            for at, event in events:
                pl.when(e == at)(event)
            body(e)

    def acts(g):
        def body(e):
            db[e, g * half:(g + 1) * half, :ff] = dot(rows_b[e], w1b[e]).astype(BF16)
            db[e, g * half:(g + 1) * half, ff:] = dot(rows_b[e], w3b[e]).astype(BF16)
        return body

    def grads(g):
        rows = slice(g * half, (g + 1) * half)

        def body(e):
            grad_hidden = dot(w2b[e], rows_b[e], NT).T
            hidden, grad_gate, grad_up = swiglu_parts(db[e, rows, :ff], db[e, rows, ff:], grad_hidden)
            db[e, rows, :ff] = grad_gate
            db[e, rows, ff:] = grad_up
            hb[e, :, rows] = hidden.T

            @pl.loop(0, dim // blk)
            def _(i):
                r = (dot(w1b[e, block(i), :], db[e, rows, :ff], NT) + dot(w3b[e, block(i), :], db[e, rows, ff:], NT)).astype(BF16)
                for p in range(2):
                    rb[p, block(i), pl.ds(pl.multiple_of(e * pairw, pairw), pairw)] = r[:, p * pairw:(p + 1) * pairw]
        return body

    def combine(p):
        q = p % 2

        @pl.loop(0, dim // blk)
        def _(i):
            s = dot(rb[q, block(i), :], mb[p])
            pb[2 * q, block(i), :] = s[:, :tok]
            pb[2 * q + 1, block(i), :] = s[:, tok:]

    def side(frm, to_slot):
        return remote(pb.at[frm], pr.at[to_slot], psend.at[to_slot], precv.at[to_slot], partner)

    def add(to_slot, terms):
        @pl.loop(0, dim // blk)
        def _(i):
            v = pr[to_slot, block(i), :]
            for t in terms:
                v = v + t[block(i), :]
            pr[to_slot, block(i), :] = v

    for c in shared_load:
        c.wait()
    act_gate = dot(xg[0], w1b[last])
    act_up = dot(xg[0], w3b[last])
    hidden, grad_gate, grad_up = swiglu_parts(act_gate.astype(BF16), act_up.astype(BF16), dot(w2b[last], yg[0], NT).T)
    dsb[:, :ff] = grad_gate
    dsb[:, ff:] = grad_up
    hsb[...] = hidden.T
    shared_out = [pltpu.make_async_copy(dsb, ds_out, osem.at[0]), pltpu.make_async_copy(hsb, hs_out, osem.at[1])]
    start(shared_out)

    @pl.loop(0, dim // blk)
    def _(i):
        shr[block(i), :] = dot(w1b[last, block(i), :], dsb[:, :ff], NT) + dot(w3b[last, block(i), :], dsb[:, ff:], NT)

    start(expert_loads[last])
    wait_recv(metas)
    pick(0, 0, 1)
    xs[1].wait_recv()
    gather(xg, 0, 0, 1, False)

    xs[2].wait_recv()
    xs[4].start()
    xs[3].start()
    ys[2].start()
    xs[6].start()
    pick(1, 2, 3)
    xs[3].wait_recv()
    gather(xg, 1, 2, 3, False)
    keep_x0 = kept(x_out, 0, 2)
    keep_x0.start()

    def have_weights(e):
        def event():
            for c in expert_loads[e]:
                c.wait()
        return event

    expert_loop(acts(0), [(e, have_weights(e)) for e in range(experts)])
    pick(2, 4, 5)
    pick(3, 6, 7)
    xs[4].wait_recv()
    xs[5].start()
    xs[6].wait_recv()
    xs[7].start()
    ys[6].start()
    keep_x0.wait()
    xs[5].wait_recv()
    gather(xg, 2, 4, 5, False)
    xs[7].wait_recv()
    gather(xg, 3, 6, 7, False)
    keep_x1 = kept(x_out, 1, 3)
    keep_x1.start()

    def near_on():
        ys[2].wait_recv()
        ys[4].start()
        ys[3].start()

    expert_loop(acts(1), [(last, near_on)])

    keep_x1.wait()
    ys[1].wait_recv()
    gather(yg, 0, 0, 1, True)
    ys[3].wait_recv()
    gather(yg, 1, 2, 3, True)
    keep_z0 = kept(z_out, 0, 4)
    keep_z0.start()

    def sides():
        ys[4].wait_recv()
        ys[5].start()
        ys[6].wait_recv()
        ys[7].start()

    expert_loop(grads(0), [(last, sides)])
    combine(0)
    to_own = side(1, 0)
    to_own.start()
    combine(1)
    to_near = side(3, 1)
    to_near.start()

    keep_z0.wait()
    ys[5].wait_recv()
    gather(yg, 2, 4, 5, True)
    ys[7].wait_recv()
    gather(yg, 3, 6, 7, True)
    keep_z1 = kept(z_out, 1, 5)
    keep_z1.start()
    own_copy = pltpu.make_async_copy(pr.at[0], own_out, osem.at[8])
    ret_near = remote(pr.at[1], ret, rsem.at[0], rsem.at[1], prv)

    def sum_near():
        to_near.wait()
        add(1, [pb.at[2]])
        ret_near.start()
        to_own.wait()
        add(0, [pb.at[0], shr])
        own_copy.start()

    expert_loop(grads(1), [(0, sum_near)])
    keep_d = [pltpu.make_async_copy(db, d_out, osem.at[6]), pltpu.make_async_copy(hb, h_out, osem.at[7])]
    start(keep_d)
    combine(2)
    to_far = side(1, 2)
    to_far.start()
    combine(3)
    to_back = side(3, 3)
    to_back.start()
    to_far.wait()
    add(2, [pb.at[0]])
    far_copy = pltpu.make_async_copy(pr.at[2], far_out, osem.at[9])
    far_copy.start()
    to_back.wait()
    add(3, [pb.at[2]])
    back_copy = pltpu.make_async_copy(pr.at[3], back_out, osem.at[10])
    back_copy.start()
    ret_near.wait()
    near_copy = pltpu.make_async_copy(ret, near_out, osem.at[11])
    near_copy.start()
    for c in shared_out + [keep_z1] + keep_d + [own_copy, far_copy, back_copy, near_copy]:
        c.wait()
    for c in list(xs.values()) + list(ys.values()) + metas:
        c.wait_send()


def layer(chips, x, dy, ids, pos, gates, weights, shared, slots):
    experts, dim, ff = weights[0].shape
    top_k, tok = ids.shape
    pairw = 2 * slots
    rows = chips * pairw
    half = 2 * pairw
    dma = pltpu.SemaphoreType.DMA
    sds = jax.ShapeDtypeStruct
    hbm = pl.BlockSpec(memory_space=pltpu.HBM)
    return pl.pallas_call(
        functools.partial(layer_kernel, chips, top_k, slots),
        name='layer',
        out_shape=(sds((experts, rows, dim), BF16), sds((experts, rows, dim), BF16), sds((experts, rows, 2 * ff), BF16), sds((experts, ff, rows), BF16),
                   sds((tok, 2 * ff), BF16), sds((ff, tok), BF16), sds((dim, tok), F32), sds((dim, tok), F32), sds((dim, tok), F32), sds((dim, tok), F32)),
        in_specs=[hbm] * 2 + [VMEM] * 3 + [hbm] * 6,
        out_specs=(hbm,) * 10,
        scratch_shapes=[
            pltpu.VMEM((8, tok, dim), BF16), pltpu.VMEM((8, tok, dim), BF16), pltpu.VMEM((8, 32, tok), F32),
            pltpu.VMEM((experts, dim, ff), BF16), pltpu.VMEM((experts, dim, ff), BF16), pltpu.VMEM((experts, ff, dim), BF16),
            pltpu.VMEM((experts, half, dim), BF16),
            pltpu.VMEM((2, dim, experts * pairw), BF16),
            pltpu.VMEM((experts, rows, 2 * ff), BF16), pltpu.VMEM((experts, ff, rows), BF16),
            pltpu.VMEM((tok, 2 * ff), BF16), pltpu.VMEM((ff, tok), BF16), pltpu.VMEM((dim, tok), F32),
            pltpu.VMEM((4, dim, tok), F32), pltpu.VMEM((4, dim, tok), F32), pltpu.VMEM((dim, tok), F32),
            pltpu.VMEM((4, experts * pairw, 2 * tok), BF16), pltpu.VMEM((4, experts * pairw, tok), F32),
            dma((2,)), dma((3, experts + 1)), dma((12,)), dma((8,)), dma((8,)), dma((8,)), dma((8,)), dma((8,)), dma((8,)), dma((4,)), dma((4,)), dma((2,)),
        ],
        compiler_params=pltpu.CompilerParams(vmem_limit_bytes=67043328, collective_id=0, has_side_effects=True),
        cost_estimate=pl.CostEstimate(flops=10 * experts * rows * dim * ff, bytes_accessed=3 * experts * dim * ff * 2, transcendentals=experts * rows * ff),
    )(x, dy, ids, pos, gates, *weights, *shared)


def last_kernel(x, z, d, h, a, b, c, g1, g3, g2, grad_x):
    ff = g1.shape[2]
    x_t = x[...].T
    g1[0] = dot(x_t, d[:, :ff])
    g3[0] = dot(x_t, d[:, ff:])
    g2[0] = dot(h[...], z[...])
    grad_x[...] = (a[...] + b[...] + c[...]).T.astype(BF16)


def shared_grads_and_sum(x, z, d, h, sums):
    tok, dim = x.shape
    ff = h.shape[0]
    blk = 512
    wide = pl.BlockSpec((tok, blk), lambda i: (0, i))
    sds = jax.ShapeDtypeStruct
    return pl.pallas_call(
        last_kernel,
        name='shared_grads_and_sum',
        grid=(dim // blk,),
        in_specs=[wide] * 2 + [pl.BlockSpec(d.shape, lambda i: (0, 0)), pl.BlockSpec(h.shape, lambda i: (0, 0))] + [pl.BlockSpec((blk, tok), lambda i: (i, 0))] * 3,
        out_specs=(pl.BlockSpec((1, blk, ff), lambda i: (0, i, 0)), pl.BlockSpec((1, blk, ff), lambda i: (0, i, 0)), pl.BlockSpec((1, ff, blk), lambda i: (0, 0, i)), wide),
        out_shape=(sds((1, dim, ff), F32), sds((1, dim, ff), F32), sds((1, ff, dim), F32), sds((tok, dim), BF16)),
        compiler_params=pltpu.CompilerParams(vmem_limit_bytes=60 * 2**20),
        cost_estimate=pl.CostEstimate(flops=6 * tok * dim * ff, bytes_accessed=12 * dim * ff, transcendentals=0),
    )(x, z, d, h, *sums)


def grad_kernel(x, z, d, h, *outs):
    g1, g3, g2 = outs[-3:]
    ff = g1.shape[2]
    x_t = x[0].T
    g1[0] = dot(x_t, d[0, :, :ff])
    g3[0] = dot(x_t, d[0, :, ff:])
    g2[0] = dot(h[0], z[0])


def weight_grads(x, z, d, h, first, count, prior):
    experts, rows, dim = x.shape
    ff = h.shape[1]
    blk = 512
    any_spec = pl.BlockSpec(memory_space=pl.ANY)
    in_specs = [pl.BlockSpec((1, rows, blk), lambda e, i: (first + e, 0, i))] * 2 + [pl.BlockSpec((1,) + a.shape[1:], lambda e, i: (first + e, 0, 0)) for a in (d, h)]
    sds = jax.ShapeDtypeStruct
    return pl.pallas_call(
        grad_kernel,
        name='weight_grads',
        grid=(count, dim // blk),
        in_specs=in_specs + [any_spec] * len(prior),
        out_specs=(pl.BlockSpec((1, blk, ff), lambda e, i: (first + e, i, 0)), pl.BlockSpec((1, blk, ff), lambda e, i: (first + e, i, 0)), pl.BlockSpec((1, ff, blk), lambda e, i: (first + e, 0, i))),
        out_shape=(sds((experts, dim, ff), F32), sds((experts, dim, ff), F32), sds((experts, ff, dim), F32)),
        input_output_aliases={4 + i: i for i in range(len(prior))},
        compiler_params=pltpu.CompilerParams(vmem_limit_bytes=60 * 2**20),
        cost_estimate=pl.CostEstimate(flops=6 * count * rows * dim * ff, bytes_accessed=count * dim * (rows * 4 + ff * 12), transcendentals=0),
    )(x, z, d, h, *prior)


def solution(mesh):
    group = mesh.shape['ep']
    cores = 2
    chips = group // cores
    token_spec = P(('dp', 'ep'), None)
    expert_spec = P('ep', None, None)
    whole_spec = P(None, None)
    grad_spec = P(('dp', 'ep'), None, None)

    assert chips == 4

    def shift(step):
        return [(c * cores + k, ((c + (step if k == 0 else -step)) % chips) * cores + k) for c in range(chips) for k in range(cores)]

    def local_backward(x_tokens, dy_tokens, expert_ids, gate_vals, slot_pos, w_gate, w_up, w_down, shared_gate, shared_up, shared_down):
        tok, top_k = expert_ids.shape
        num_experts = w_gate.shape[0] * group
        ff = w_gate.shape[2]
        capacity = (3 * tok * top_k + 2 * num_experts - 1) // (2 * num_experts)
        slots = pl.cdiv(capacity, 64) * 64
        x, z, d, h, ds, hs, own_sum, ret_near, far_sum, back_sum = layer(chips, x_tokens, dy_tokens, expert_ids.T, slot_pos.T, gate_vals.T, (w_gate, w_up, w_down), (shared_gate, shared_up, shared_down), slots)
        via = lax.ppermute(far_sum, 'ep', shift(1))
        half_experts = w_gate.shape[0] // 2
        first = weight_grads(x, z, d, h, 0, half_experts, ())
        via, first = lax.optimization_barrier((via, first))
        ret_back = lax.ppermute(back_sum + via, 'ep', shift(1))
        g1, g3, g2 = weight_grads(x, z, d, h, half_experts, w_gate.shape[0] - half_experts, first)
        gsg, gsu, gsd, grad_x = shared_grads_and_sum(x_tokens, dy_tokens, ds, hs, (own_sum, ret_near, ret_back))
        return grad_x, g1, g3, g2, gsg, gsu, gsd

    return jax.shard_map(local_backward, mesh=mesh, in_specs=(token_spec, token_spec, token_spec, token_spec, token_spec, expert_spec, expert_spec, expert_spec, whole_spec, whole_spec, whole_spec), out_specs=(token_spec, grad_spec, grad_spec, grad_spec, grad_spec, grad_spec, grad_spec), check_vma=False)
```

```python
import functools

import jax
import jax.numpy as jnp
from jax import lax
from jax.experimental import pallas as pl
from jax.experimental.pallas import tpu as pltpu
from jax.sharding import PartitionSpec as P

BF16 = jnp.bfloat16
F32 = jnp.float32
NN = (((1,), (0,)), ((), ()))
NT = (((1,), (1,)), ((), ()))
TN = (((0,), (0,)), ((), ()))
ANY = pl.BlockSpec(memory_space=pl.ANY)
VMEM = pl.BlockSpec(memory_space=pltpu.VMEM)
SMEM = pl.BlockSpec(memory_space=pltpu.SMEM)


def dot(a, b, dims=NN):
    return lax.dot_general(a, b, dims, preferred_element_type=F32)


def swiglu_parts(act_gate, act_up, grad_hidden):
    gate_f32 = act_gate.astype(F32)
    up_f32 = act_up.astype(F32)
    sigma = jax.nn.sigmoid(gate_f32)
    silu_gate = gate_f32 * sigma
    hidden = (silu_gate * up_f32).astype(BF16)
    grad_gate = (grad_hidden * up_f32 * sigma * (1.0 + gate_f32 * (1.0 - sigma))).astype(BF16)
    grad_up = (grad_hidden * silu_gate).astype(BF16)
    return hidden, grad_gate, grad_up


def layer_kernel(chips, top_k, slots, x, dy, ids, pos, gates, w1, w3, w2, sg, su, sd,
                 x_out, z_out, d_out, h_out, ds_out, hs_out, own_out, near_out, far_out, back_out,
                 xg, yg, meta, w1b, w3b, w2b, rows_b, rb, db, hb, dsb, hsb, shr, pb, pr, ret, mb, gb,
                 lsem, wsem, osem, msend, mrecv, xsend, xrecv, ysend, yrecv, psend, precv, rsem):
    experts, dim, ff = w1.shape
    tok = x.shape[0]
    pairw = 2 * slots
    half = 2 * pairw
    me = lax.axis_index('ep')
    core = lax.rem(me, 2)
    chip = me // 2
    sign = 1 - 2 * core

    def device(step, other):
        return lax.rem(chip + sign * step + chips, chips) * 2 + (1 - core if other else core)

    partner, nxt, prv = device(0, True), device(1, False), device(-1, False)
    peers = [(partner, 1), (nxt, 2), (device(1, True), 3), (device(2, False), 4), (device(2, True), 5), (prv, 6), (device(-1, True), 7)]

    def remote(src, dst, ss, rs, to):
        return pltpu.make_async_remote_copy(src_ref=src, dst_ref=dst, send_sem=ss, recv_sem=rs, device_id={'ep': to}, device_id_type=pl.DeviceIdType.MESH)

    def send_x(frm, slot, to):
        return remote(xg.at[frm], xg.at[slot], xsend.at[slot], xrecv.at[slot], to)

    def send_y(frm, slot, to):
        return remote(yg.at[frm], yg.at[slot], ysend.at[slot], yrecv.at[slot], to)

    def start(copies):
        for c in copies:
            c.start()

    own = [pltpu.make_async_copy(x, xg.at[0], lsem.at[0]), pltpu.make_async_copy(dy, yg.at[0], lsem.at[1])]
    start(own)
    barrier = pltpu.get_barrier_semaphore()
    for to, _ in peers:
        pl.semaphore_signal(barrier, inc=1, device_id={'ep': to}, device_id_type=pl.DeviceIdType.MESH)
    pl.semaphore_wait(barrier, len(peers))

    routes = ((0, 1, partner), (0, 2, nxt), (2, 3, partner), (2, 4, nxt), (4, 5, partner), (0, 6, prv), (6, 7, partner))
    xs = {slot: send_x(frm, slot, to) for frm, slot, to in routes}
    ys = {slot: send_y(frm, slot, to) for frm, slot, to in routes}
    meta[0, :top_k] = jnp.where(pos[...] >= 0, ids[...] * slots + pos[...], -1).astype(F32)
    meta[0, 16:16 + top_k] = gates[...]
    metas = [remote(meta.at[0], meta.at[s], msend.at[s], mrecv.at[s], to) for to, s in peers]
    own[0].wait()
    start(metas)
    xs[2].start()
    xs[1].start()
    own[1].wait()
    ys[2].start()
    ys[1].start()

    loads13 = [[pltpu.make_async_copy(w1.at[e], w1b.at[e], wsem.at[0, e]), pltpu.make_async_copy(w3.at[e], w3b.at[e], wsem.at[1, e])] for e in range(experts)]
    loads2 = [pltpu.make_async_copy(w2.at[e], w2b.at[e], wsem.at[2, e]) for e in range(experts)]
    part = sd.shape[1] // experts
    shared_load = [pltpu.make_async_copy(sg, rb.at[0], lsem.at[2]), pltpu.make_async_copy(su, rb.at[1], lsem.at[3])]
    shared_load += [pltpu.make_async_copy(sd.at[:, i * part:(i + 1) * part], hb.at[i], lsem.at[4 + i]) for i in range(experts)]
    last = experts - 1
    start(shared_load)
    for e in range(experts):
        start(loads13[e])
    start(loads2)
    blk = 512

    def block(i):
        return pl.ds(pl.multiple_of(i * blk, blk), blk)

    def wait_recv(copies):
        for c in copies:
            c.wait_recv()

    def pick(p, a, b):
        mb[p] = jnp.zeros(mb.shape[1:], BF16)
        for s, slot in enumerate((a, b)):
            info = meta[slot]
            row = lax.broadcasted_iota(jnp.int32, (experts * slots, tok), 0)
            key = (row + me * (experts * slots)).astype(F32)
            hit = jnp.zeros((experts * slots, tok), F32)
            gate = jnp.zeros((experts * slots, tok), F32)
            for j in range(top_k):
                eq = key == info[j:j + 1, :]
                hit = jnp.where(eq, 1.0, hit)
                gate = jnp.where(eq, info[16 + j:17 + j, :], gate)
            hit = hit.astype(BF16)
            gate = jnp.broadcast_to(jnp.sum(gate, axis=1, keepdims=True), (experts * slots, tok))
            for e in range(experts):
                dst = slice(e * pairw + s * slots, e * pairw + (s + 1) * slots)
                mb[p, dst, s * tok:(s + 1) * tok] = hit[e * slots:(e + 1) * slots]
                gb[p, dst, :] = gate[e * slots:(e + 1) * slots]

    def gather(src, p, a, b, gated):
        col = 256
        at = (p % 2) * pairw
        for i in range(dim // col):
            cols = slice(i * col, (i + 1) * col)
            r = dot(mb[p], jnp.concatenate([src[a, :, cols], src[b, :, cols]], axis=0))
            if gated:
                r = r * jnp.concatenate([gb[p]] * (col // tok), axis=1)
            r = r.astype(BF16)
            for e in range(experts):
                rows_b[e, at:at + pairw, cols] = r[e * pairw:(e + 1) * pairw]

    def kept(out, g, n):
        return pltpu.make_async_copy(rows_b, out.at[:, g * half:(g + 1) * half], osem.at[n])

    def expert_loop(body, events):
        @pl.loop(0, experts)
        def _(e):
            for at, event in events:
                pl.when(e == at)(event)
            body(e)

    def acts(g):
        def body(e):
            db[e, g * half:(g + 1) * half, :ff] = dot(rows_b[e], w1b[e]).astype(BF16)
            db[e, g * half:(g + 1) * half, ff:] = dot(rows_b[e], w3b[e]).astype(BF16)
        return body

    def grads(g, events):
        rows = slice(g * half, (g + 1) * half)

        def hidden_grads(e):
            grad_hidden = dot(w2b[e], rows_b[e], NT).T
            hidden, grad_gate, grad_up = swiglu_parts(db[e, rows, :ff], db[e, rows, ff:], grad_hidden)
            db[e, rows, :ff] = grad_gate
            db[e, rows, ff:] = grad_up
            hb[e, :, rows] = hidden.T

        def input_grads(e):
            for i in range(dim // blk):
                part = slice(i * blk, (i + 1) * blk)
                r = (dot(w1b[e, part, :], db[e, rows, :ff], NT) + dot(w3b[e, part, :], db[e, rows, ff:], NT)).astype(BF16)
                for p in range(2):
                    rb[p, part, e * pairw:(e + 1) * pairw] = r[:, p * pairw:(p + 1) * pairw]

        hidden_grads(0)
        for e in range(experts):
            for at, event in events:
                if at == e:
                    event()
            if e + 1 < experts:
                hidden_grads(e + 1)
            input_grads(e)

    def combine(p):
        q = p % 2

        for i in range(dim // blk):
            part = slice(i * blk, (i + 1) * blk)
            s = dot(rb[q, part, :], mb[p])
            pb[2 * q, part, :] = s[:, :tok]
            pb[2 * q + 1, part, :] = s[:, tok:]

    def side(frm, to_slot):
        return remote(pb.at[frm], pr.at[to_slot], psend.at[to_slot], precv.at[to_slot], partner)

    def add(to_slot, terms):
        @pl.loop(0, dim // blk)
        def _(i):
            v = pr[to_slot, block(i), :]
            for t in terms:
                v = v + t[block(i), :]
            pr[to_slot, block(i), :] = v

    for c in shared_load:
        c.wait()
    act_gate = dot(xg[0], rb[0])
    act_up = dot(xg[0], rb[1])
    grad_hidden = dot(hb[0], yg[0, :, :part], NT)
    for i in range(1, experts):
        grad_hidden += dot(hb[i], yg[0, :, i * part:(i + 1) * part], NT)
    hidden, grad_gate, grad_up = swiglu_parts(act_gate.astype(BF16), act_up.astype(BF16), grad_hidden.T)
    dsb[:, :ff] = grad_gate
    dsb[:, ff:] = grad_up
    hsb[...] = hidden.T
    shared_out = [pltpu.make_async_copy(dsb, ds_out, osem.at[0]), pltpu.make_async_copy(hsb, hs_out, osem.at[1])]
    start(shared_out)
    for i in range(dim // blk):
        rows = slice(i * blk, (i + 1) * blk)
        shr[rows, :] = dot(rb[0, rows, :], dsb[:, :ff], NT) + dot(rb[1, rows, :], dsb[:, ff:], NT)

    wait_recv(metas)
    pick(0, 0, 1)
    xs[1].wait_recv()
    gather(xg, 0, 0, 1, False)

    xs[2].wait_recv()
    xs[4].start()
    xs[3].start()
    pick(1, 2, 3)
    xs[3].wait_recv()
    xs[6].start()
    ys[6].start()
    gather(xg, 1, 2, 3, False)
    keep_x0 = kept(x_out, 0, 2)
    keep_x0.start()

    def have_weights(e):
        def event():
            for c in loads13[e]:
                c.wait()
        return event

    def near_on():
        ys[2].wait_recv()
        ys[4].start()
        ys[3].start()

    expert_loop(acts(0), [(e, have_weights(e)) for e in range(experts)] + [(last, near_on)])
    pick(2, 4, 5)
    pick(3, 6, 7)
    keep_x0.wait()
    ys[1].wait_recv()
    gather(yg, 0, 0, 1, True)
    ys[3].wait_recv()
    gather(yg, 1, 2, 3, True)
    keep_z0 = kept(z_out, 0, 4)
    keep_z0.start()
    for c in loads2:
        c.wait()

    def x_sides():
        xs[4].wait_recv()
        xs[5].start()
        xs[6].wait_recv()
        xs[7].start()

    grads(0, [(last, x_sides)])
    combine(0)
    to_own = side(1, 0)
    to_own.start()
    combine(1)
    to_near = side(3, 1)
    to_near.start()

    keep_z0.wait()
    xs[5].wait_recv()
    gather(xg, 2, 4, 5, False)
    xs[7].wait_recv()
    gather(xg, 3, 6, 7, False)
    keep_x1 = kept(x_out, 1, 3)
    keep_x1.start()
    own_copy = pltpu.make_async_copy(pr.at[0], own_out, osem.at[8])
    ret_near = remote(pr.at[1], ret, rsem.at[0], rsem.at[1], prv)

    def sum_near():
        to_near.wait()
        add(1, [pb.at[2]])
        ret_near.start()
        to_own.wait()
        add(0, [pb.at[0], shr])
        own_copy.start()

    expert_loop(acts(1), [(1, sum_near)])
    ys[4].wait_recv()
    ys[5].start()
    ys[6].wait_recv()
    ys[7].start()
    keep_x1.wait()
    ys[5].wait_recv()
    gather(yg, 2, 4, 5, True)
    ys[7].wait_recv()
    gather(yg, 3, 6, 7, True)
    keep_z1 = kept(z_out, 1, 5)
    keep_z1.start()
    grads(1, [])
    keep_d = [pltpu.make_async_copy(db, d_out, osem.at[6]), pltpu.make_async_copy(hb, h_out, osem.at[7])]
    start(keep_d)
    combine(2)
    to_far = side(1, 2)
    to_far.start()
    combine(3)
    to_back = side(3, 3)
    to_back.start()
    to_far.wait()
    add(2, [pb.at[0]])
    far_copy = pltpu.make_async_copy(pr.at[2], far_out, osem.at[9])
    far_copy.start()
    to_back.wait()
    add(3, [pb.at[2]])
    back_copy = pltpu.make_async_copy(pr.at[3], back_out, osem.at[10])
    back_copy.start()
    ret_near.wait()
    near_copy = pltpu.make_async_copy(ret, near_out, osem.at[11])
    near_copy.start()
    for c in shared_out + [keep_z1] + keep_d + [own_copy, far_copy, back_copy, near_copy]:
        c.wait()
    for c in list(xs.values()) + list(ys.values()) + metas:
        c.wait_send()


def layer(chips, x, dy, ids, pos, gates, weights, shared, slots):
    experts, dim, ff = weights[0].shape
    top_k, tok = ids.shape
    pairw = 2 * slots
    rows = chips * pairw
    half = 2 * pairw
    dma = pltpu.SemaphoreType.DMA
    sds = jax.ShapeDtypeStruct
    hbm = pl.BlockSpec(memory_space=pltpu.HBM)
    return pl.pallas_call(
        functools.partial(layer_kernel, chips, top_k, slots),
        name='layer',
        out_shape=(sds((experts, rows, dim), BF16), sds((experts, rows, dim), BF16), sds((experts, rows, 2 * ff), BF16), sds((experts, ff, rows), BF16),
                   sds((tok, 2 * ff), BF16), sds((ff, tok), BF16), sds((dim, tok), F32), sds((dim, tok), F32), sds((dim, tok), F32), sds((dim, tok), F32)),
        in_specs=[hbm] * 2 + [VMEM] * 3 + [hbm] * 6,
        out_specs=(hbm,) * 10,
        scratch_shapes=[
            pltpu.VMEM((8, tok, dim), BF16), pltpu.VMEM((8, tok, dim), BF16), pltpu.VMEM((8, 32, tok), F32),
            pltpu.VMEM((experts, dim, ff), BF16), pltpu.VMEM((experts, dim, ff), BF16), pltpu.VMEM((experts, ff, dim), BF16),
            pltpu.VMEM((experts, half, dim), BF16),
            pltpu.VMEM((2, dim, experts * pairw), BF16),
            pltpu.VMEM((experts, rows, 2 * ff), BF16), pltpu.VMEM((experts, ff, rows), BF16),
            pltpu.VMEM((tok, 2 * ff), BF16), pltpu.VMEM((ff, tok), BF16), pltpu.VMEM((dim, tok), F32),
            pltpu.VMEM((4, dim, tok), F32), pltpu.VMEM((4, dim, tok), F32), pltpu.VMEM((dim, tok), F32),
            pltpu.VMEM((4, experts * pairw, 2 * tok), BF16), pltpu.VMEM((4, experts * pairw, tok), F32),
            dma((4 + experts,)), dma((3, experts)), dma((12,)), dma((8,)), dma((8,)), dma((8,)), dma((8,)), dma((8,)), dma((8,)), dma((4,)), dma((4,)), dma((2,)),
        ],
        compiler_params=pltpu.CompilerParams(vmem_limit_bytes=67043328, collective_id=0, has_side_effects=True),
        cost_estimate=pl.CostEstimate(flops=10 * experts * rows * dim * ff, bytes_accessed=3 * experts * dim * ff * 2, transcendentals=experts * rows * ff),
    )(x, dy, ids, pos, gates, *weights, *shared)


def last_kernel(x, z, d, h, a, b, c, g1, g3, g2, grad_x):
    ff = g1.shape[2]
    x_t = x[...].T
    g1[0] = dot(x_t, d[:, :ff])
    g3[0] = dot(x_t, d[:, ff:])
    g2[0] = dot(h[...], z[...])
    grad_x[...] = (a[...] + b[...] + c[...]).T.astype(BF16)


def shared_grads_and_sum(x, z, d, h, sums):
    tok, dim = x.shape
    ff = h.shape[0]
    blk = 512
    wide = pl.BlockSpec((tok, blk), lambda i: (0, i))
    sds = jax.ShapeDtypeStruct
    return pl.pallas_call(
        last_kernel,
        name='shared_grads_and_sum',
        grid=(dim // blk,),
        in_specs=[wide] * 2 + [pl.BlockSpec(d.shape, lambda i: (0, 0)), pl.BlockSpec(h.shape, lambda i: (0, 0))] + [pl.BlockSpec((blk, tok), lambda i: (i, 0))] * 3,
        out_specs=(pl.BlockSpec((1, blk, ff), lambda i: (0, i, 0)), pl.BlockSpec((1, blk, ff), lambda i: (0, i, 0)), pl.BlockSpec((1, ff, blk), lambda i: (0, 0, i)), wide),
        out_shape=(sds((1, dim, ff), F32), sds((1, dim, ff), F32), sds((1, ff, dim), F32), sds((tok, dim), BF16)),
        compiler_params=pltpu.CompilerParams(vmem_limit_bytes=60 * 2**20),
        cost_estimate=pl.CostEstimate(flops=6 * tok * dim * ff, bytes_accessed=12 * dim * ff, transcendentals=0),
    )(x, z, d, h, *sums)


def grad_kernel(x, z, d, h, *outs):
    g1, g3, g2 = outs[-3:]
    ff = g1.shape[2]
    x_t = x[0].T
    g1[0] = dot(x_t, d[0, :, :ff])
    g3[0] = dot(x_t, d[0, :, ff:])
    g2[0] = dot(h[0], z[0])


def weight_grads(x, z, d, h, first, count, prior):
    experts, rows, dim = x.shape
    ff = h.shape[1]
    blk = 512
    any_spec = pl.BlockSpec(memory_space=pl.ANY)
    in_specs = [pl.BlockSpec((1, rows, blk), lambda e, i: (first + e, 0, i))] * 2 + [pl.BlockSpec((1,) + a.shape[1:], lambda e, i: (first + e, 0, 0)) for a in (d, h)]
    sds = jax.ShapeDtypeStruct
    return pl.pallas_call(
        grad_kernel,
        name='weight_grads',
        grid=(count, dim // blk),
        in_specs=in_specs + [any_spec] * len(prior),
        out_specs=(pl.BlockSpec((1, blk, ff), lambda e, i: (first + e, i, 0)), pl.BlockSpec((1, blk, ff), lambda e, i: (first + e, i, 0)), pl.BlockSpec((1, ff, blk), lambda e, i: (first + e, 0, i))),
        out_shape=(sds((experts, dim, ff), F32), sds((experts, dim, ff), F32), sds((experts, ff, dim), F32)),
        input_output_aliases={4 + i: i for i in range(len(prior))},
        compiler_params=pltpu.CompilerParams(vmem_limit_bytes=60 * 2**20),
        cost_estimate=pl.CostEstimate(flops=6 * count * rows * dim * ff, bytes_accessed=count * dim * (rows * 4 + ff * 12), transcendentals=0),
    )(x, z, d, h, *prior)


def solution(mesh):
    group = mesh.shape['ep']
    cores = 2
    chips = group // cores
    token_spec = P(('dp', 'ep'), None)
    expert_spec = P('ep', None, None)
    whole_spec = P(None, None)
    grad_spec = P(('dp', 'ep'), None, None)

    assert chips == 4

    def shift(step):
        return [(c * cores + k, ((c + (step if k == 0 else -step)) % chips) * cores + k) for c in range(chips) for k in range(cores)]

    def local_backward(x_tokens, dy_tokens, expert_ids, gate_vals, slot_pos, w_gate, w_up, w_down, shared_gate, shared_up, shared_down):
        tok, top_k = expert_ids.shape
        num_experts = w_gate.shape[0] * group
        ff = w_gate.shape[2]
        capacity = (3 * tok * top_k + 2 * num_experts - 1) // (2 * num_experts)
        slots = pl.cdiv(capacity, 64) * 64
        x, z, d, h, ds, hs, own_sum, ret_near, far_sum, back_sum = layer(chips, x_tokens, dy_tokens, expert_ids.T, slot_pos.T, gate_vals.T, (w_gate, w_up, w_down), (shared_gate, shared_up, shared_down), slots)
        via = lax.ppermute(far_sum, 'ep', shift(1))
        half_experts = w_gate.shape[0] // 2
        first = weight_grads(x, z, d, h, 0, half_experts, ())
        via, first = lax.optimization_barrier((via, first))
        ret_back = lax.ppermute(back_sum + via, 'ep', shift(1))
        g1, g3, g2 = weight_grads(x, z, d, h, half_experts, w_gate.shape[0] - half_experts, first)
        gsg, gsu, gsd, grad_x = shared_grads_and_sum(x_tokens, dy_tokens, ds, hs, (own_sum, ret_near, ret_back))
        return grad_x, g1, g3, g2, gsg, gsu, gsd

    return jax.shard_map(local_backward, mesh=mesh, in_specs=(token_spec, token_spec, token_spec, token_spec, token_spec, expert_spec, expert_spec, expert_spec, whole_spec, whole_spec, whole_spec), out_specs=(token_spec, grad_spec, grad_spec, grad_spec, grad_spec, grad_spec, grad_spec), check_vma=False)
```

```python
import functools

import jax
import jax.numpy as jnp
from jax import lax
from jax.experimental import pallas as pl
from jax.experimental.pallas import tpu as pltpu
from jax.sharding import PartitionSpec as P

BF16 = jnp.bfloat16
F32 = jnp.float32
NN = (((1,), (0,)), ((), ()))
NT = (((1,), (1,)), ((), ()))
TN = (((0,), (0,)), ((), ()))
ANY = pl.BlockSpec(memory_space=pl.ANY)
VMEM = pl.BlockSpec(memory_space=pltpu.VMEM)
SMEM = pl.BlockSpec(memory_space=pltpu.SMEM)


def dot(a, b, dims=NN):
    return lax.dot_general(a, b, dims, preferred_element_type=F32)


def swiglu_parts(act_gate, act_up, grad_hidden):
    gate_f32 = act_gate.astype(F32)
    up_f32 = act_up.astype(F32)
    sigma = jax.nn.sigmoid(gate_f32)
    silu_gate = gate_f32 * sigma
    hidden = (silu_gate * up_f32).astype(BF16)
    grad_gate = (grad_hidden * up_f32 * sigma * (1.0 + gate_f32 * (1.0 - sigma))).astype(BF16)
    grad_up = (grad_hidden * silu_gate).astype(BF16)
    return hidden, grad_gate, grad_up


def layer_kernel(chips, top_k, slots, x, dy, ids, pos, gates, w1, w3, w2, sg, su, sd,
                 x_out, z_out, d_out, h_out, ds_out, hs_out, own_out, near_out, far_out, back_out,
                 xg, yg, meta, w1b, w3b, w2b, rows_b, rb, db, hb, dsb, hsb, shr, pb, pr, ret, mb, gb,
                 lsem, wsem, osem, msend, mrecv, xsend, xrecv, ysend, yrecv, psend, precv, rsem):
    experts, dim, ff = w1.shape
    tok = x.shape[0]
    pairw = 2 * slots
    half = 2 * pairw
    me = lax.axis_index('ep')
    core = lax.rem(me, 2)
    chip = me // 2
    sign = 1 - 2 * core

    def device(step, other):
        return lax.rem(chip + sign * step + chips, chips) * 2 + (1 - core if other else core)

    partner, nxt, prv = device(0, True), device(1, False), device(-1, False)
    peers = [(partner, 1), (nxt, 2), (device(1, True), 3), (device(2, False), 4), (device(2, True), 5), (prv, 6), (device(-1, True), 7)]

    def remote(src, dst, ss, rs, to):
        return pltpu.make_async_remote_copy(src_ref=src, dst_ref=dst, send_sem=ss, recv_sem=rs, device_id={'ep': to}, device_id_type=pl.DeviceIdType.MESH)

    def send_x(frm, slot, to):
        return remote(xg.at[frm], xg.at[slot], xsend.at[slot], xrecv.at[slot], to)

    def send_y(frm, slot, to):
        return remote(yg.at[frm], yg.at[slot], ysend.at[slot], yrecv.at[slot], to)

    def start(copies):
        for c in copies:
            c.start()

    own = [pltpu.make_async_copy(x, xg.at[0], lsem.at[0]), pltpu.make_async_copy(dy, yg.at[0], lsem.at[1])]
    start(own)
    barrier = pltpu.get_barrier_semaphore()
    for to, _ in peers:
        pl.semaphore_signal(barrier, inc=1, device_id={'ep': to}, device_id_type=pl.DeviceIdType.MESH)
    pl.semaphore_wait(barrier, len(peers))

    routes = ((0, 1, partner), (0, 2, nxt), (2, 3, partner), (2, 4, nxt), (4, 5, partner), (0, 6, prv), (6, 7, partner))
    xs = {slot: send_x(frm, slot, to) for frm, slot, to in routes}
    ys = {slot: send_y(frm, slot, to) for frm, slot, to in routes}
    meta[0, :top_k] = jnp.where(pos[...] >= 0, ids[...] * slots + pos[...], -1).astype(F32)
    meta[0, 16:16 + top_k] = gates[...]
    metas = [remote(meta.at[0], meta.at[s], msend.at[s], mrecv.at[s], to) for to, s in peers]
    own[0].wait()
    start(metas)
    xs[2].start()
    xs[1].start()
    own[1].wait()
    ys[2].start()
    ys[1].start()

    loads13 = [[pltpu.make_async_copy(w1.at[e], w1b.at[e], wsem.at[0, e]), pltpu.make_async_copy(w3.at[e], w3b.at[e], wsem.at[1, e])] for e in range(experts)]
    loads2 = [pltpu.make_async_copy(w2.at[e], w2b.at[e], wsem.at[2, e]) for e in range(experts)]
    part = sd.shape[1] // experts
    shared_load = [pltpu.make_async_copy(sg, rb.at[0], lsem.at[2]), pltpu.make_async_copy(su, rb.at[1], lsem.at[3])]
    shared_load += [pltpu.make_async_copy(sd.at[:, i * part:(i + 1) * part], hb.at[i], lsem.at[4 + i]) for i in range(experts)]
    last = experts - 1
    start(shared_load)
    for e in range(experts):
        start(loads13[e])
    start(loads2)
    blk = 512

    def block(i):
        return pl.ds(pl.multiple_of(i * blk, blk), blk)

    def wait_recv(copies):
        for c in copies:
            c.wait_recv()

    def pick(p, a, b):
        mb[p] = jnp.zeros(mb.shape[1:], BF16)
        for s, slot in enumerate((a, b)):
            info = meta[slot]
            row = lax.broadcasted_iota(jnp.int32, (experts * slots, tok), 0)
            key = (row + me * (experts * slots)).astype(F32)
            hit = jnp.zeros((experts * slots, tok), F32)
            gate = jnp.zeros((experts * slots, tok), F32)
            for j in range(top_k):
                eq = key == info[j:j + 1, :]
                hit = jnp.where(eq, 1.0, hit)
                gate = jnp.where(eq, info[16 + j:17 + j, :], gate)
            hit = hit.astype(BF16)
            gate = jnp.broadcast_to(jnp.sum(gate, axis=1, keepdims=True), (experts * slots, tok))
            for e in range(experts):
                dst = slice(e * pairw + s * slots, e * pairw + (s + 1) * slots)
                mb[p, dst, s * tok:(s + 1) * tok] = hit[e * slots:(e + 1) * slots]
                gb[p, dst, :] = gate[e * slots:(e + 1) * slots]

    def gather(src, p, a, b, gated):
        col = 256
        at = (p % 2) * pairw
        for i in range(dim // col):
            cols = slice(i * col, (i + 1) * col)
            r = dot(mb[p], jnp.concatenate([src[a, :, cols], src[b, :, cols]], axis=0))
            if gated:
                r = r * jnp.concatenate([gb[p]] * (col // tok), axis=1)
            r = r.astype(BF16)
            for e in range(experts):
                rows_b[e, at:at + pairw, cols] = r[e * pairw:(e + 1) * pairw]

    def kept(out, g, n):
        return pltpu.make_async_copy(rows_b, out.at[:, g * half:(g + 1) * half], osem.at[n])

    def expert_loop(body, events):
        @pl.loop(0, experts)
        def _(e):
            for at, event in events:
                pl.when(e == at)(event)
            body(e)

    def acts(g):
        def body(e):
            db[e, g * half:(g + 1) * half, :ff] = dot(rows_b[e], w1b[e]).astype(BF16)
            db[e, g * half:(g + 1) * half, ff:] = dot(rows_b[e], w3b[e]).astype(BF16)
        return body

    def grads(g, events):
        rows = slice(g * half, (g + 1) * half)

        def hidden_grads(e):
            grad_hidden = dot(w2b[e], rows_b[e], NT).T
            hidden, grad_gate, grad_up = swiglu_parts(db[e, rows, :ff], db[e, rows, ff:], grad_hidden)
            db[e, rows, :ff] = grad_gate
            db[e, rows, ff:] = grad_up
            hb[e, :, rows] = hidden.T

        def input_grads(e):
            for i in range(dim // blk):
                part = slice(i * blk, (i + 1) * blk)
                r = (dot(w1b[e, part, :], db[e, rows, :ff], NT) + dot(w3b[e, part, :], db[e, rows, ff:], NT)).astype(BF16)
                for p in range(2):
                    rb[p, part, e * pairw:(e + 1) * pairw] = r[:, p * pairw:(p + 1) * pairw]

        hidden_grads(0)
        for e in range(experts):
            for at, event in events:
                if at == e:
                    event()
            if e + 1 < experts:
                hidden_grads(e + 1)
            input_grads(e)

    def combine(p):
        q = p % 2

        for i in range(dim // blk):
            part = slice(i * blk, (i + 1) * blk)
            s = dot(rb[q, part, :], mb[p])
            pb[2 * q, part, :] = s[:, :tok]
            pb[2 * q + 1, part, :] = s[:, tok:]

    def side(frm, to_slot):
        return remote(pb.at[frm], pr.at[to_slot], psend.at[to_slot], precv.at[to_slot], partner)

    def add(to_slot, terms):
        @pl.loop(0, dim // blk)
        def _(i):
            v = pr[to_slot, block(i), :]
            for t in terms:
                v = v + t[block(i), :]
            pr[to_slot, block(i), :] = v

    for c in shared_load:
        c.wait()
    act_gate = dot(xg[0], rb[0])
    act_up = dot(xg[0], rb[1])
    grad_hidden = dot(hb[0], yg[0, :, :part], NT)
    for i in range(1, experts):
        grad_hidden += dot(hb[i], yg[0, :, i * part:(i + 1) * part], NT)
    hidden, grad_gate, grad_up = swiglu_parts(act_gate.astype(BF16), act_up.astype(BF16), grad_hidden.T)
    dsb[:, :ff] = grad_gate
    dsb[:, ff:] = grad_up
    hsb[...] = hidden.T
    shared_out = [pltpu.make_async_copy(dsb, ds_out, osem.at[0]), pltpu.make_async_copy(hsb, hs_out, osem.at[1])]
    start(shared_out)
    for i in range(dim // blk):
        rows = slice(i * blk, (i + 1) * blk)
        shr[rows, :] = dot(rb[0, rows, :], dsb[:, :ff], NT) + dot(rb[1, rows, :], dsb[:, ff:], NT)

    wait_recv(metas)
    pick(0, 0, 1)
    xs[1].wait_recv()
    gather(xg, 0, 0, 1, False)

    xs[2].wait_recv()
    xs[4].start()
    xs[3].start()
    pick(1, 2, 3)
    xs[3].wait_recv()
    xs[6].start()
    ys[6].start()
    gather(xg, 1, 2, 3, False)
    keep_x0 = kept(x_out, 0, 2)
    keep_x0.start()

    def have_weights(e):
        def event():
            for c in loads13[e]:
                c.wait()
        return event

    def near_on():
        ys[2].wait_recv()
        ys[4].start()
        ys[3].start()

    expert_loop(acts(0), [(e, have_weights(e)) for e in range(experts)] + [(last, near_on)])
    pick(2, 4, 5)
    pick(3, 6, 7)
    keep_x0.wait()
    ys[1].wait_recv()
    gather(yg, 0, 0, 1, True)
    ys[3].wait_recv()
    gather(yg, 1, 2, 3, True)
    keep_z0 = kept(z_out, 0, 4)
    keep_z0.start()
    for c in loads2:
        c.wait()

    def x_sides():
        xs[4].wait_recv()
        xs[5].start()
        xs[6].wait_recv()
        xs[7].start()

    grads(0, [(last, x_sides)])
    combine(0)
    to_own = side(1, 0)
    to_own.start()
    combine(1)
    to_near = side(3, 1)
    to_near.start()

    keep_z0.wait()
    xs[5].wait_recv()
    gather(xg, 2, 4, 5, False)
    xs[7].wait_recv()
    gather(xg, 3, 6, 7, False)
    keep_x1 = kept(x_out, 1, 3)
    keep_x1.start()
    own_copy = pltpu.make_async_copy(pr.at[0], own_out, osem.at[8])
    ret_near = remote(pr.at[1], ret, rsem.at[0], rsem.at[1], prv)

    def sum_near():
        to_near.wait()
        add(1, [pb.at[2]])
        ret_near.start()
        to_own.wait()
        add(0, [pb.at[0], shr])
        own_copy.start()

    expert_loop(acts(1), [(1, sum_near)])
    ys[4].wait_recv()
    ys[5].start()
    ys[6].wait_recv()
    ys[7].start()
    keep_x1.wait()
    ys[5].wait_recv()
    gather(yg, 2, 4, 5, True)
    ys[7].wait_recv()
    gather(yg, 3, 6, 7, True)
    keep_z1 = kept(z_out, 1, 5)
    keep_z1.start()
    grads(1, [])
    keep_d = [pltpu.make_async_copy(db, d_out, osem.at[6]), pltpu.make_async_copy(hb, h_out, osem.at[7])]
    start(keep_d)
    combine(2)
    to_far = side(1, 2)
    to_far.start()
    combine(3)
    to_back = side(3, 3)
    to_back.start()
    to_far.wait()
    add(2, [pb.at[0]])
    far_copy = pltpu.make_async_copy(pr.at[2], far_out, osem.at[9])
    far_copy.start()
    to_back.wait()
    add(3, [pb.at[2]])
    back_copy = pltpu.make_async_copy(pr.at[3], back_out, osem.at[10])
    back_copy.start()
    ret_near.wait()
    near_copy = pltpu.make_async_copy(ret, near_out, osem.at[11])
    near_copy.start()
    for c in shared_out + [keep_z1] + keep_d + [own_copy, far_copy, back_copy, near_copy]:
        c.wait()
    for c in list(xs.values()) + list(ys.values()) + metas:
        c.wait_send()


def layer(chips, x, dy, ids, pos, gates, weights, shared, slots):
    experts, dim, ff = weights[0].shape
    top_k, tok = ids.shape
    pairw = 2 * slots
    rows = chips * pairw
    half = 2 * pairw
    dma = pltpu.SemaphoreType.DMA
    sds = jax.ShapeDtypeStruct
    hbm = pl.BlockSpec(memory_space=pltpu.HBM)
    return pl.pallas_call(
        functools.partial(layer_kernel, chips, top_k, slots),
        name='layer',
        out_shape=(sds((experts, rows, dim), BF16), sds((experts, rows, dim), BF16), sds((experts, rows, 2 * ff), BF16), sds((experts, ff, rows), BF16),
                   sds((tok, 2 * ff), BF16), sds((ff, tok), BF16), sds((dim, tok), F32), sds((dim, tok), F32), sds((dim, tok), F32), sds((dim, tok), F32)),
        in_specs=[hbm] * 2 + [VMEM] * 3 + [hbm] * 6,
        out_specs=(hbm,) * 10,
        scratch_shapes=[
            pltpu.VMEM((8, tok, dim), BF16), pltpu.VMEM((8, tok, dim), BF16), pltpu.VMEM((8, 32, tok), F32),
            pltpu.VMEM((experts, dim, ff), BF16), pltpu.VMEM((experts, dim, ff), BF16), pltpu.VMEM((experts, ff, dim), BF16),
            pltpu.VMEM((experts, half, dim), BF16),
            pltpu.VMEM((2, dim, experts * pairw), BF16),
            pltpu.VMEM((experts, rows, 2 * ff), BF16), pltpu.VMEM((experts, ff, rows), BF16),
            pltpu.VMEM((tok, 2 * ff), BF16), pltpu.VMEM((ff, tok), BF16), pltpu.VMEM((dim, tok), F32),
            pltpu.VMEM((4, dim, tok), F32), pltpu.VMEM((4, dim, tok), F32), pltpu.VMEM((dim, tok), F32),
            pltpu.VMEM((4, experts * pairw, 2 * tok), BF16), pltpu.VMEM((4, experts * pairw, tok), F32),
            dma((4 + experts,)), dma((3, experts)), dma((12,)), dma((8,)), dma((8,)), dma((8,)), dma((8,)), dma((8,)), dma((8,)), dma((4,)), dma((4,)), dma((2,)),
        ],
        compiler_params=pltpu.CompilerParams(vmem_limit_bytes=67043328, collective_id=0, has_side_effects=True),
        cost_estimate=pl.CostEstimate(flops=10 * experts * rows * dim * ff, bytes_accessed=3 * experts * dim * ff * 2, transcendentals=experts * rows * ff),
    )(x, dy, ids, pos, gates, *weights, *shared)


def grad_kernel(first, count, shared, prior, *refs):
    n_in = 4 + (4 if shared else 0)
    ins, refs = refs[:n_in], refs[n_in + prior:]
    n_out = 3 + (3 if shared else 0)
    outs, (xb, zb, db, hb, sx, sz, sd, sh, g1b, g3b, g2b, xsem, dsem, ssem, osem) = refs[:n_out], refs[n_out:]
    x, z, d, h = ins[:4]
    ff = h.shape[1]
    dim = x.shape[2]
    blk = g1b.shape[1]
    blocks = dim // blk

    def cols(i):
        return pl.ds(pl.multiple_of(i * blk, blk), blk)

    def small(n):
        b = n % 2
        return [pltpu.make_async_copy(d.at[first + n], db.at[b], dsem.at[0, b]), pltpu.make_async_copy(h.at[first + n], hb.at[b], dsem.at[1, b])]

    def wide(n, i):
        b = n % 2
        return [pltpu.make_async_copy(x.at[first + n, :, cols(i)], xb.at[b, :, cols(i)], xsem.at[0, b, i]),
                pltpu.make_async_copy(z.at[first + n, :, cols(i)], zb.at[b, :, cols(i)], xsem.at[1, b, i])]

    def fetch(n):
        for c in small(n):
            c.start()
        for i in range(blocks):
            for c in wide(n, i):
                c.start()

    def stores(dst, e, i):
        return [pltpu.make_async_copy(g1b.at[i], dst[0].at[e, cols(i), :], osem.at[0, i]),
                pltpu.make_async_copy(g3b.at[i], dst[1].at[e, cols(i), :], osem.at[1, i]),
                pltpu.make_async_copy(g2b.at[i], dst[2].at[e, :, cols(i)], osem.at[2, i])]

    def item(dst, e, waits, xv, zv, dv, hv, busy):
        @pl.loop(0, blocks)
        def _(i):
            for c in waits(i):
                c.wait()
            if busy:
                for c in stores(dst, e, i):
                    c.wait()
            x_t = xv[:, cols(i)].T
            g1b[i] = dot(x_t, dv[:, :ff])
            g3b[i] = dot(x_t, dv[:, ff:])
            g2b[i] = dot(hv[...], zv[:, cols(i)])
            for c in stores(dst, e, i):
                c.start()

    if shared:
        own = [pltpu.make_async_copy(a, b, ssem.at[i]) for i, (a, b) in enumerate(zip(ins[4:], (sx, sz, sd, sh)))]
        for c in own:
            c.start()
        fetch(0)
        for c in own:
            c.wait()
        item(outs[3:], 0, lambda i: [], sx, sz, sd, sh, False)
    else:
        fetch(0)
    for n in range(count):
        if n + 1 < count:
            fetch(n + 1)
        for c in small(n):
            c.wait()
        b = n % 2
        item(outs[:3], first + n, functools.partial(wide, n), xb.at[b], zb.at[b], db.at[b], hb.at[b], shared or n > 0)

    @pl.loop(0, blocks)
    def _(i):
        for c in stores(outs[:3], first, i):
            c.wait()


def weight_grads(x, z, d, h, first, count, shared=(), prior=()):
    experts, rows, dim = x.shape
    ff = h.shape[1]
    tok = shared[0].shape[0] if shared else 16
    srow = shared[3].shape[1] if shared else 128
    blk = 512
    blocks = dim // blk
    any_spec = pl.BlockSpec(memory_space=pltpu.HBM)
    sds = jax.ShapeDtypeStruct
    dma = pltpu.SemaphoreType.DMA
    out_shape = (sds((experts, dim, ff), F32), sds((experts, dim, ff), F32), sds((experts, ff, dim), F32))
    if shared:
        out_shape += (sds((1, dim, ff), F32), sds((1, dim, ff), F32), sds((1, ff, dim), F32))
    return pl.pallas_call(
        functools.partial(grad_kernel, first, count, bool(shared), len(prior)),
        name='weight_grads',
        in_specs=[any_spec] * (4 + len(shared) + len(prior)),
        out_specs=(any_spec,) * len(out_shape),
        out_shape=out_shape,
        input_output_aliases={4 + len(shared) + i: i for i in range(len(prior))},
        scratch_shapes=[
            pltpu.VMEM((2, rows, dim), BF16), pltpu.VMEM((2, rows, dim), BF16), pltpu.VMEM((2, rows, 2 * ff), BF16), pltpu.VMEM((2, ff, rows), BF16),
            pltpu.VMEM((tok, dim), BF16), pltpu.VMEM((tok, dim), BF16), pltpu.VMEM((tok, 2 * ff), BF16), pltpu.VMEM((ff, srow), BF16),
            pltpu.VMEM((blocks, blk, ff), F32), pltpu.VMEM((blocks, blk, ff), F32), pltpu.VMEM((blocks, ff, blk), F32),
            dma((2, 2, blocks)), dma((2, 2)), dma((4,)), dma((3, blocks)),
        ],
        compiler_params=pltpu.CompilerParams(vmem_limit_bytes=60 * 2**20),
        cost_estimate=pl.CostEstimate(flops=6 * count * rows * dim * ff, bytes_accessed=count * dim * (rows * 4 + ff * 12), transcendentals=0),
    )(x, z, d, h, *shared, *prior)


def final_kernel(a, b, c, out):
    out[...] = (a[...] + b[...] + c[...]).T.astype(BF16)


def final_sum(*terms):
    dim, tok = terms[0].shape
    blk = 1024
    return pl.pallas_call(
        final_kernel,
        name='final_sum',
        grid=(dim // blk,),
        in_specs=[pl.BlockSpec((blk, tok), lambda i: (i, 0))] * 3,
        out_specs=pl.BlockSpec((tok, blk), lambda i: (0, i)),
        out_shape=jax.ShapeDtypeStruct((tok, dim), BF16),
        cost_estimate=pl.CostEstimate(flops=5 * dim * tok, bytes_accessed=dim * tok * 14, transcendentals=0),
    )(*terms)


def solution(mesh):
    group = mesh.shape['ep']
    cores = 2
    chips = group // cores
    token_spec = P(('dp', 'ep'), None)
    expert_spec = P('ep', None, None)
    whole_spec = P(None, None)
    grad_spec = P(('dp', 'ep'), None, None)

    assert chips == 4

    def shift(step):
        return [(c * cores + k, ((c + (step if k == 0 else -step)) % chips) * cores + k) for c in range(chips) for k in range(cores)]

    def local_backward(x_tokens, dy_tokens, expert_ids, gate_vals, slot_pos, w_gate, w_up, w_down, shared_gate, shared_up, shared_down):
        tok, top_k = expert_ids.shape
        num_experts = w_gate.shape[0] * group
        ff = w_gate.shape[2]
        capacity = (3 * tok * top_k + 2 * num_experts - 1) // (2 * num_experts)
        slots = pl.cdiv(capacity, 64) * 64
        x, z, d, h, ds, hs, own_sum, ret_near, far_sum, back_sum = layer(chips, x_tokens, dy_tokens, expert_ids.T, slot_pos.T, gate_vals.T, (w_gate, w_up, w_down), (shared_gate, shared_up, shared_down), slots)
        via = lax.ppermute(far_sum, 'ep', shift(1))
        half_experts = w_gate.shape[0] // 2
        *first, gsg, gsu, gsd = weight_grads(x, z, d, h, 0, half_experts, (x_tokens, dy_tokens, ds, hs))
        via, first, gsg = lax.optimization_barrier((via, first, gsg))
        ret_back = lax.ppermute(back_sum + via, 'ep', shift(1))
        g1, g3, g2 = weight_grads(x, z, d, h, half_experts, w_gate.shape[0] - half_experts, (), tuple(first))
        grad_x = final_sum(own_sum, ret_near, ret_back)
        return grad_x, g1, g3, g2, gsg, gsu, gsd

    return jax.shard_map(local_backward, mesh=mesh, in_specs=(token_spec, token_spec, token_spec, token_spec, token_spec, expert_spec, expert_spec, expert_spec, whole_spec, whole_spec, whole_spec), out_specs=(token_spec, grad_spec, grad_spec, grad_spec, grad_spec, grad_spec, grad_spec), check_vma=False)
```

```python
import functools

import jax
import jax.numpy as jnp
from jax import lax
from jax.experimental import pallas as pl
from jax.experimental.pallas import tpu as pltpu
from jax.sharding import PartitionSpec as P

BF16 = jnp.bfloat16
F32 = jnp.float32
NN = (((1,), (0,)), ((), ()))
NT = (((1,), (1,)), ((), ()))
TN = (((0,), (0,)), ((), ()))
ANY = pl.BlockSpec(memory_space=pl.ANY)
VMEM = pl.BlockSpec(memory_space=pltpu.VMEM)
SMEM = pl.BlockSpec(memory_space=pltpu.SMEM)


def dot(a, b, dims=NN):
    return lax.dot_general(a, b, dims, preferred_element_type=F32)


def swiglu_parts(act_gate, act_up, grad_hidden):
    gate_f32 = act_gate.astype(F32)
    up_f32 = act_up.astype(F32)
    sigma = jax.nn.sigmoid(gate_f32)
    silu_gate = gate_f32 * sigma
    hidden = (silu_gate * up_f32).astype(BF16)
    grad_gate = (grad_hidden * up_f32 * sigma * (1.0 + gate_f32 * (1.0 - sigma))).astype(BF16)
    grad_up = (grad_hidden * silu_gate).astype(BF16)
    return hidden, grad_gate, grad_up


def layer_kernel(chips, top_k, slots, x, dy, ids, pos, gates, w1, w3, w2, sg, su, sd,
                 x_out, z_out, d_out, h_out, ds_out, hs_out, own_out, near_out, far_out, back_out,
                 xg, yg, meta, w1b, w3b, w2b, rows_b, rb, db, hb, dsb, hsb, shr, pb, pr, mb, gb,
                 lsem, wsem, osem, msend, mrecv, xsend, xrecv, ysend, yrecv, psend, precv, rsem):
    experts, dim, ff = w1.shape
    tok = x.shape[0]
    pairw = 2 * slots
    half = 2 * pairw
    me = lax.axis_index('ep')
    core = lax.rem(me, 2)
    chip = me // 2
    sign = 1 - 2 * core

    def device(step, other):
        return lax.rem(chip + sign * step + chips, chips) * 2 + (1 - core if other else core)

    partner, nxt, prv = device(0, True), device(1, False), device(-1, False)
    peers = [(partner, 1), (nxt, 2), (device(1, True), 3), (device(2, False), 4), (device(2, True), 5), (prv, 6), (device(-1, True), 7)]

    def remote(src, dst, ss, rs, to):
        return pltpu.make_async_remote_copy(src_ref=src, dst_ref=dst, send_sem=ss, recv_sem=rs, device_id={'ep': to}, device_id_type=pl.DeviceIdType.MESH)

    def send_x(frm, slot, to):
        return remote(xg.at[frm], xg.at[slot], xsend.at[slot], xrecv.at[slot], to)

    def send_y(frm, slot, to):
        return remote(yg.at[frm], yg.at[slot], ysend.at[slot], yrecv.at[slot], to)

    def start(copies):
        for c in copies:
            c.start()

    own = [pltpu.make_async_copy(x, xg.at[0], lsem.at[0]), pltpu.make_async_copy(dy, yg.at[0], lsem.at[1])]
    start(own)
    barrier = pltpu.get_barrier_semaphore()
    for to, _ in peers:
        pl.semaphore_signal(barrier, inc=1, device_id={'ep': to}, device_id_type=pl.DeviceIdType.MESH)
    pl.semaphore_wait(barrier, len(peers))

    routes = ((0, 1, partner), (0, 2, nxt), (2, 3, partner), (2, 4, nxt), (4, 5, partner), (0, 6, prv), (6, 7, partner))
    xs = {slot: send_x(frm, slot, to) for frm, slot, to in routes}
    ys = {slot: send_y(frm, slot, to) for frm, slot, to in routes}
    meta[0, :top_k] = jnp.where(pos[...] >= 0, ids[...] * slots + pos[...], -1).astype(F32)
    meta[0, 16:16 + top_k] = gates[...]
    metas = [remote(meta.at[0], meta.at[s], msend.at[s], mrecv.at[s], to) for to, s in peers]
    own[0].wait()
    start(metas)
    xs[2].start()
    xs[1].start()
    own[1].wait()
    ys[2].start()
    ys[1].start()

    loads13 = [[pltpu.make_async_copy(w1.at[e], w1b.at[e], wsem.at[0, e]), pltpu.make_async_copy(w3.at[e], w3b.at[e], wsem.at[1, e])] for e in range(experts)]
    loads2 = [pltpu.make_async_copy(w2.at[e], w2b.at[e], wsem.at[2, e]) for e in range(experts)]
    part = sd.shape[1] // experts
    shared_load = [pltpu.make_async_copy(sg, rb.at[0], lsem.at[2]), pltpu.make_async_copy(su, rb.at[1], lsem.at[3])]
    shared_load += [pltpu.make_async_copy(sd.at[:, i * part:(i + 1) * part], hb.at[i], lsem.at[4 + i]) for i in range(experts)]
    last = experts - 1
    start(shared_load)
    for e in range(experts):
        start(loads13[e])
    start(loads2)
    blk = 512

    def block(i):
        return pl.ds(pl.multiple_of(i * blk, blk), blk)

    def wait_recv(copies):
        for c in copies:
            c.wait_recv()

    def pick(p, a, b):
        mb[p] = jnp.zeros(mb.shape[1:], BF16)
        for s, slot in enumerate((a, b)):
            info = meta[slot]
            row = lax.broadcasted_iota(jnp.int32, (experts * slots, tok), 0)
            key = (row + me * (experts * slots)).astype(F32)
            hit = jnp.zeros((experts * slots, tok), F32)
            gate = jnp.zeros((experts * slots, tok), F32)
            for j in range(top_k):
                eq = key == info[j:j + 1, :]
                hit = jnp.where(eq, 1.0, hit)
                gate = jnp.where(eq, info[16 + j:17 + j, :], gate)
            hit = hit.astype(BF16)
            gate = jnp.broadcast_to(jnp.sum(gate, axis=1, keepdims=True), (experts * slots, tok))
            for e in range(experts):
                dst = slice(e * pairw + s * slots, e * pairw + (s + 1) * slots)
                mb[p, dst, s * tok:(s + 1) * tok] = hit[e * slots:(e + 1) * slots]
                gb[p, dst, :] = gate[e * slots:(e + 1) * slots]

    def gather(src, p, a, b, gated):
        col = 256
        at = (p % 2) * pairw
        for i in range(dim // col):
            cols = slice(i * col, (i + 1) * col)
            r = dot(mb[p], jnp.concatenate([src[a, :, cols], src[b, :, cols]], axis=0))
            if gated:
                r = r * jnp.concatenate([gb[p]] * (col // tok), axis=1)
            r = r.astype(BF16)
            for e in range(experts):
                rows_b[e, at:at + pairw, cols] = r[e * pairw:(e + 1) * pairw]

    def kept(out, g, n):
        return pltpu.make_async_copy(rows_b, out.at[:, g * half:(g + 1) * half], osem.at[n])

    def expert_loop(body, events):
        @pl.loop(0, experts)
        def _(e):
            for at, event in events:
                pl.when(e == at)(event)
            body(e)

    def acts(g):
        def body(e):
            db[e, g * half:(g + 1) * half, :ff] = dot(rows_b[e], w1b[e]).astype(BF16)
            db[e, g * half:(g + 1) * half, ff:] = dot(rows_b[e], w3b[e]).astype(BF16)
        return body

    def grads(g, events):
        rows = slice(g * half, (g + 1) * half)

        def hidden_grads(e):
            grad_hidden = dot(w2b[e], rows_b[e], NT).T
            hidden, grad_gate, grad_up = swiglu_parts(db[e, rows, :ff], db[e, rows, ff:], grad_hidden)
            db[e, rows, :ff] = grad_gate
            db[e, rows, ff:] = grad_up
            hb[e, :, rows] = hidden.T

        def input_grads(e):
            for i in range(dim // blk):
                part = slice(i * blk, (i + 1) * blk)
                r = (dot(w1b[e, part, :], db[e, rows, :ff], NT) + dot(w3b[e, part, :], db[e, rows, ff:], NT)).astype(BF16)
                for p in range(2):
                    rb[p, part, e * pairw:(e + 1) * pairw] = r[:, p * pairw:(p + 1) * pairw]

        hidden_grads(0)
        for e in range(experts):
            for at, event in events:
                if at == e:
                    event()
            if e + 1 < experts:
                hidden_grads(e + 1)
            input_grads(e)

    def combine(p):
        q = p % 2

        for i in range(dim // blk):
            part = slice(i * blk, (i + 1) * blk)
            s = dot(rb[q, part, :], mb[p])
            pb[2 * q, part, :] = s[:, :tok]
            pb[2 * q + 1, part, :] = s[:, tok:]

    def side(frm, to_slot):
        return remote(pb.at[frm], pr.at[to_slot], psend.at[to_slot], precv.at[to_slot], partner)

    def add(to_slot, terms):
        @pl.loop(0, dim // blk)
        def _(i):
            v = pr[to_slot, block(i), :]
            for t in terms:
                v = v + t[block(i), :]
            pr[to_slot, block(i), :] = v

    wait_recv(metas[:1])
    pick(0, 0, 1)

    for c in shared_load:
        c.wait()
    act_gate = dot(xg[0], rb[0])
    act_up = dot(xg[0], rb[1])
    grad_hidden = dot(hb[0], yg[0, :, :part], NT)
    for i in range(1, experts):
        grad_hidden += dot(hb[i], yg[0, :, i * part:(i + 1) * part], NT)
    hidden, grad_gate, grad_up = swiglu_parts(act_gate.astype(BF16), act_up.astype(BF16), grad_hidden.T)
    dsb[:, :ff] = grad_gate
    dsb[:, ff:] = grad_up
    hsb[...] = hidden.T
    shared_out = [pltpu.make_async_copy(dsb, ds_out, osem.at[0]), pltpu.make_async_copy(hsb, hs_out, osem.at[1])]
    start(shared_out)
    for i in range(dim // blk):
        rows = slice(i * blk, (i + 1) * blk)
        shr[rows, :] = dot(rb[0, rows, :], dsb[:, :ff], NT) + dot(rb[1, rows, :], dsb[:, ff:], NT)

    xs[1].wait_recv()
    gather(xg, 0, 0, 1, False)
    wait_recv(metas[1:])
    pick(1, 2, 3)

    xs[2].wait_recv()
    xs[4].start()
    xs[3].start()
    pick(2, 4, 5)
    pick(3, 6, 7)
    xs[3].wait_recv()
    xs[6].start()
    ys[6].start()
    gather(xg, 1, 2, 3, False)
    keep_x0 = kept(x_out, 0, 2)
    keep_x0.start()

    def have_weights(e):
        def event():
            for c in loads13[e]:
                c.wait()
        return event

    def near_on():
        ys[2].wait_recv()
        ys[4].start()
        ys[3].start()

    expert_loop(acts(0), [(e, have_weights(e)) for e in range(experts)] + [(last, near_on)])
    keep_x0.wait()
    ys[1].wait_recv()
    gather(yg, 0, 0, 1, True)
    ys[3].wait_recv()
    gather(yg, 1, 2, 3, True)
    keep_z0 = kept(z_out, 0, 4)
    keep_z0.start()
    for c in loads2:
        c.wait()

    def x_sides():
        xs[4].wait_recv()
        xs[5].start()
        xs[6].wait_recv()
        xs[7].start()

    grads(0, [(last, x_sides)])
    combine(0)
    to_own = side(1, 0)
    to_own.start()
    combine(1)
    to_near = side(3, 1)
    to_near.start()

    keep_z0.wait()
    xs[5].wait_recv()
    gather(xg, 2, 4, 5, False)
    xs[7].wait_recv()
    gather(xg, 3, 6, 7, False)
    keep_x1 = kept(x_out, 1, 3)
    keep_x1.start()
    own_copy = pltpu.make_async_copy(pr.at[0], own_out, osem.at[8])
    ret_near = remote(pr.at[1], near_out, rsem.at[0], rsem.at[1], prv)

    def sum_near():
        to_near.wait()
        add(1, [pb.at[2]])
        ret_near.start()
        to_own.wait()
        add(0, [pb.at[0], shr])
        own_copy.start()

    expert_loop(acts(1), [(1, sum_near)])
    ys[4].wait_recv()
    ys[5].start()
    ys[6].wait_recv()
    ys[7].start()
    keep_x1.wait()
    ys[5].wait_recv()
    gather(yg, 2, 4, 5, True)
    ys[7].wait_recv()
    gather(yg, 3, 6, 7, True)
    keep_z1 = kept(z_out, 1, 5)
    keep_z1.start()
    grads(1, [])
    keep_d = [pltpu.make_async_copy(db, d_out, osem.at[6]), pltpu.make_async_copy(hb, h_out, osem.at[7])]
    start(keep_d)
    combine(2)
    to_far = side(1, 2)
    to_far.start()
    combine(3)
    to_back = side(3, 3)
    to_back.start()
    to_far.wait()
    add(2, [pb.at[0]])
    far_copy = pltpu.make_async_copy(pr.at[2], far_out, osem.at[9])
    far_copy.start()
    to_back.wait()
    add(3, [pb.at[2]])
    back_copy = pltpu.make_async_copy(pr.at[3], back_out, osem.at[10])
    back_copy.start()
    ret_near.wait()
    for c in shared_out + [keep_z1] + keep_d + [own_copy, far_copy, back_copy]:
        c.wait()
    for c in list(xs.values()) + list(ys.values()) + metas:
        c.wait_send()


def layer(chips, x, dy, ids, pos, gates, weights, shared, slots):
    experts, dim, ff = weights[0].shape
    top_k, tok = ids.shape
    pairw = 2 * slots
    rows = chips * pairw
    half = 2 * pairw
    dma = pltpu.SemaphoreType.DMA
    sds = jax.ShapeDtypeStruct
    hbm = pl.BlockSpec(memory_space=pltpu.HBM)
    return pl.pallas_call(
        functools.partial(layer_kernel, chips, top_k, slots),
        name='layer',
        out_shape=(sds((experts, rows, dim), BF16), sds((experts, rows, dim), BF16), sds((experts, rows, 2 * ff), BF16), sds((experts, ff, rows), BF16),
                   sds((tok, 2 * ff), BF16), sds((ff, tok), BF16), sds((dim, tok), F32), sds((dim, tok), F32), sds((dim, tok), F32), sds((dim, tok), F32)),
        in_specs=[hbm] * 2 + [VMEM] * 3 + [hbm] * 6,
        out_specs=(hbm,) * 10,
        scratch_shapes=[
            pltpu.VMEM((8, tok, dim), BF16), pltpu.VMEM((8, tok, dim), BF16), pltpu.VMEM((8, 32, tok), F32),
            pltpu.VMEM((experts, dim, ff), BF16), pltpu.VMEM((experts, dim, ff), BF16), pltpu.VMEM((experts, ff, dim), BF16),
            pltpu.VMEM((experts, half, dim), BF16),
            pltpu.VMEM((2, dim, experts * pairw), BF16),
            pltpu.VMEM((experts, rows, 2 * ff), BF16), pltpu.VMEM((experts, ff, rows), BF16),
            pltpu.VMEM((tok, 2 * ff), BF16), pltpu.VMEM((ff, tok), BF16), pltpu.VMEM((dim, tok), F32),
            pltpu.VMEM((4, dim, tok), F32), pltpu.VMEM((4, dim, tok), F32),
            pltpu.VMEM((4, experts * pairw, 2 * tok), BF16), pltpu.VMEM((4, experts * pairw, tok), F32),
            dma((4 + experts,)), dma((3, experts)), dma((12,)), dma((8,)), dma((8,)), dma((8,)), dma((8,)), dma((8,)), dma((8,)), dma((4,)), dma((4,)), dma((2,)),
        ],
        compiler_params=pltpu.CompilerParams(vmem_limit_bytes=67043328, collective_id=0, has_side_effects=True),
        cost_estimate=pl.CostEstimate(flops=10 * experts * rows * dim * ff, bytes_accessed=3 * experts * dim * ff * 2, transcendentals=experts * rows * ff),
    )(x, dy, ids, pos, gates, *weights, *shared)


def grad_kernel(first, count, shared, prior, *refs):
    n_in = 8
    ins, refs = refs[:n_in], refs[n_in + prior:]
    n_out = 6
    outs, (xb, zb, db, hb, sx, sz, sd, sh, g1b, g3b, g2b, dsem, ssem, osem) = refs[:n_out], refs[n_out:]
    x, z, d, h = ins[:4]
    ff = h.shape[1]
    dim = x.shape[2]
    blk = g1b.shape[1]
    blocks = dim // blk
    fblk = ff // blocks

    def cols(i):
        return pl.ds(pl.multiple_of(i * blk, blk), blk)

    def inputs(n):
        b = n % 2
        return [pltpu.make_async_copy(a.at[first + n], v.at[b], dsem.at[k, b]) for k, (a, v) in enumerate(((d, db), (x, xb), (h, hb), (z, zb)))]

    def fetch(n):
        for c in inputs(n):
            c.start()

    def rows(i):
        return pl.ds(pl.multiple_of(i * fblk, fblk), fblk)

    def stores(dst, e, i):
        return [pltpu.make_async_copy(g1b.at[i], dst[0].at[e, cols(i), :], osem.at[0, i]),
                pltpu.make_async_copy(g3b.at[i], dst[1].at[e, cols(i), :], osem.at[1, i]),
                pltpu.make_async_copy(g2b.at[i], dst[2].at[e, rows(i), :], osem.at[2, i])]

    def item(dst, e, span, xv, zv, dv, hv, busy):
        @pl.loop(*span)
        def _(i):
            @pl.when((i >= busy[0]) & (i < busy[1]))
            def _():
                for c in stores(dst, e, i):
                    c.wait()
            x_t = xv[:, cols(i)].T
            g1b[i] = dot(x_t, dv[:, :ff])
            g3b[i] = dot(x_t, dv[:, ff:])
            g2b[i] = dot(hv[rows(i), :], zv[...])
            for c in stores(dst, e, i):
                c.start()

    own = [pltpu.make_async_copy(a, b, ssem.at[i]) for i, (a, b) in enumerate(zip(ins[4:], (sx, sz, sd, sh)))]
    for c in own:
        c.start()
    fetch(0)
    for c in own:
        c.wait()
    item(outs[3:], 0, shared, sx, sz, sd, sh, (0, 0))
    for n in range(count):
        if n + 1 < count:
            fetch(n + 1)
        for c in inputs(n):
            c.wait()
        b = n % 2
        item(outs[:3], first + n, (0, blocks), xb.at[b], zb.at[b], db.at[b], hb.at[b], (0, blocks) if n else shared)

    @pl.loop(0, blocks)
    def _(i):
        for c in stores(outs[:3], first, i):
            c.wait()


def weight_grads(x, z, d, h, shared, first, count, span, prior=()):
    experts, rows, dim = x.shape
    ff = h.shape[1]
    tok = shared[0].shape[0]
    blk = 1024
    blocks = dim // blk
    span = tuple(blocks * n // 4 for n in span)
    hbm = pl.BlockSpec(memory_space=pltpu.HBM)
    sds = jax.ShapeDtypeStruct
    dma = pltpu.SemaphoreType.DMA
    out_shape = (sds((experts, dim, ff), F32), sds((experts, dim, ff), F32), sds((experts, ff, dim), F32),
                 sds((1, dim, ff), F32), sds((1, dim, ff), F32), sds((1, ff, dim), F32))
    return pl.pallas_call(
        functools.partial(grad_kernel, first, count, span, len(prior)),
        name='weight_grads',
        in_specs=[hbm] * (8 + len(prior)),
        out_specs=(hbm,) * 6,
        out_shape=out_shape,
        input_output_aliases={8 + i: i for i in range(len(prior))},
        scratch_shapes=[
            pltpu.VMEM((2, rows, dim), BF16), pltpu.VMEM((2, rows, dim), BF16), pltpu.VMEM((2, rows, 2 * ff), BF16), pltpu.VMEM((2, ff, rows), BF16),
            pltpu.VMEM((tok, dim), BF16), pltpu.VMEM((tok, dim), BF16), pltpu.VMEM((tok, 2 * ff), BF16), pltpu.VMEM((ff, tok), BF16),
            pltpu.VMEM((blocks, blk, ff), F32), pltpu.VMEM((blocks, blk, ff), F32), pltpu.VMEM((blocks, ff // blocks, dim), F32),
            dma((4, 2)), dma((4,)), dma((3, blocks)),
        ],
        compiler_params=pltpu.CompilerParams(vmem_limit_bytes=60 * 2**20),
        cost_estimate=pl.CostEstimate(flops=6 * count * rows * dim * ff, bytes_accessed=count * dim * (rows * 4 + ff * 12), transcendentals=0),
    )(x, z, d, h, *shared, *prior)


def final_kernel(a, b, c, out):
    out[...] = (a[...] + b[...] + c[...]).T.astype(BF16)


def final_sum(*terms):
    dim, tok = terms[0].shape
    blk = 1024
    return pl.pallas_call(
        final_kernel,
        name='final_sum',
        grid=(dim // blk,),
        in_specs=[pl.BlockSpec((blk, tok), lambda i: (i, 0))] * 3,
        out_specs=pl.BlockSpec((tok, blk), lambda i: (0, i)),
        out_shape=jax.ShapeDtypeStruct((tok, dim), BF16),
        cost_estimate=pl.CostEstimate(flops=5 * dim * tok, bytes_accessed=dim * tok * 14, transcendentals=0),
    )(*terms)


def solution(mesh):
    group = mesh.shape['ep']
    cores = 2
    chips = group // cores
    token_spec = P(('dp', 'ep'), None)
    expert_spec = P('ep', None, None)
    whole_spec = P(None, None)
    grad_spec = P(('dp', 'ep'), None, None)

    assert chips == 4

    def shift(step):
        return [(c * cores + k, ((c + (step if k == 0 else -step)) % chips) * cores + k) for c in range(chips) for k in range(cores)]

    def local_backward(x_tokens, dy_tokens, expert_ids, gate_vals, slot_pos, w_gate, w_up, w_down, shared_gate, shared_up, shared_down):
        tok, top_k = expert_ids.shape
        num_experts = w_gate.shape[0] * group
        ff = w_gate.shape[2]
        capacity = (3 * tok * top_k + 2 * num_experts - 1) // (2 * num_experts)
        slots = pl.cdiv(capacity, 64) * 64
        x, z, d, h, ds, hs, own_sum, ret_near, far_sum, back_sum = layer(chips, x_tokens, dy_tokens, expert_ids.T, slot_pos.T, gate_vals.T, (w_gate, w_up, w_down), (shared_gate, shared_up, shared_down), slots)
        via = lax.ppermute(far_sum, 'ep', shift(1))
        half_experts = w_gate.shape[0] // 2
        shared = (x_tokens, dy_tokens, ds, hs)
        first = weight_grads(x, z, d, h, shared, 0, half_experts, (0, 2))
        via, first = lax.optimization_barrier((via, first))
        ret_back = lax.ppermute(back_sum + via, 'ep', shift(1))
        g1, g3, g2, gsg, gsu, gsd = weight_grads(x, z, d, h, shared, half_experts, w_gate.shape[0] - half_experts, (2, 4), tuple(first))
        grad_x = final_sum(own_sum, ret_near, ret_back)
        return grad_x, g1, g3, g2, gsg, gsu, gsd

    return jax.shard_map(local_backward, mesh=mesh, in_specs=(token_spec, token_spec, token_spec, token_spec, token_spec, expert_spec, expert_spec, expert_spec, whole_spec, whole_spec, whole_spec), out_specs=(token_spec, grad_spec, grad_spec, grad_spec, grad_spec, grad_spec, grad_spec), check_vma=False)
```

```python
import functools

import jax
import jax.numpy as jnp
from jax import lax
from jax.experimental import pallas as pl
from jax.experimental.pallas import tpu as pltpu
from jax.sharding import PartitionSpec as P

BF16 = jnp.bfloat16
F32 = jnp.float32
NN = (((1,), (0,)), ((), ()))
NT = (((1,), (1,)), ((), ()))
TN = (((0,), (0,)), ((), ()))
ANY = pl.BlockSpec(memory_space=pl.ANY)
VMEM = pl.BlockSpec(memory_space=pltpu.VMEM)
SMEM = pl.BlockSpec(memory_space=pltpu.SMEM)


def dot(a, b, dims=NN):
    return lax.dot_general(a, b, dims, preferred_element_type=F32)


def swiglu_parts(act_gate, act_up, grad_hidden):
    gate_f32 = act_gate.astype(F32)
    up_f32 = act_up.astype(F32)
    sigma = jax.nn.sigmoid(gate_f32)
    silu_gate = gate_f32 * sigma
    hidden = (silu_gate * up_f32).astype(BF16)
    grad_gate = (grad_hidden * up_f32 * sigma * (1.0 + gate_f32 * (1.0 - sigma))).astype(BF16)
    grad_up = (grad_hidden * silu_gate).astype(BF16)
    return hidden, grad_gate, grad_up


def layer_kernel(chips, top_k, slots, x, dy, ids, pos, gates, w1, w3, w2, sg, su, sd,
                 x_out, z_out, d_out, h_out, ds_out, hs_out, own_out, near_out, far_out, back_out,
                 xg, yg, meta, w1b, w3b, w2b, rows_b, rb, db, hb, dsb, hsb, shr, pb, pr, mb, gb,
                 lsem, wsem, osem, msend, mrecv, xsend, xrecv, ysend, yrecv, psend, precv, rsem):
    experts, dim, ff = w1.shape
    tok = x.shape[0]
    pairw = 2 * slots
    half = 2 * pairw
    me = lax.axis_index('ep')
    core = lax.rem(me, 2)
    chip = me // 2
    sign = 1 - 2 * core

    def device(step, other):
        return lax.rem(chip + sign * step + chips, chips) * 2 + (1 - core if other else core)

    partner, nxt, prv = device(0, True), device(1, False), device(-1, False)
    peers = [(partner, 1), (nxt, 2), (device(1, True), 3), (device(2, False), 4), (device(2, True), 5), (prv, 6), (device(-1, True), 7)]

    def remote(src, dst, ss, rs, to):
        return pltpu.make_async_remote_copy(src_ref=src, dst_ref=dst, send_sem=ss, recv_sem=rs, device_id={'ep': to}, device_id_type=pl.DeviceIdType.MESH)

    def send_x(frm, slot, to):
        return remote(xg.at[frm], xg.at[slot], xsend.at[slot], xrecv.at[slot], to)

    def send_y(frm, slot, to):
        return remote(yg.at[frm], yg.at[slot], ysend.at[slot], yrecv.at[slot], to)

    def start(copies):
        for c in copies:
            c.start()

    own = [pltpu.make_async_copy(x, xg.at[0], lsem.at[0]), pltpu.make_async_copy(dy, yg.at[0], lsem.at[1])]
    start(own)
    barrier = pltpu.get_barrier_semaphore()
    for to, _ in peers:
        pl.semaphore_signal(barrier, inc=1, device_id={'ep': to}, device_id_type=pl.DeviceIdType.MESH)
    pl.semaphore_wait(barrier, len(peers))

    routes = ((0, 1, partner), (0, 2, nxt), (2, 3, partner), (2, 4, nxt), (4, 5, partner), (0, 6, prv), (6, 7, partner))
    xs = {slot: send_x(frm, slot, to) for frm, slot, to in routes}
    ys = {slot: send_y(frm, slot, to) for frm, slot, to in routes}
    meta[0, :top_k] = jnp.where(pos[...] >= 0, ids[...] * slots + pos[...], -1).astype(F32)
    meta[0, 16:16 + top_k] = gates[...]
    metas = [remote(meta.at[0], meta.at[s], msend.at[s], mrecv.at[s], to) for to, s in peers]
    own[0].wait()
    start(metas)
    xs[2].start()
    xs[1].start()
    own[1].wait()
    ys[2].start()
    ys[1].start()

    loads13 = [[pltpu.make_async_copy(w1.at[e], w1b.at[e], wsem.at[0, e]), pltpu.make_async_copy(w3.at[e], w3b.at[e], wsem.at[1, e])] for e in range(experts)]
    loads2 = [pltpu.make_async_copy(w2.at[e], w2b.at[e], wsem.at[2, e]) for e in range(experts)]
    part = sd.shape[1] // experts
    shared_load = [pltpu.make_async_copy(sg, rb.at[0], lsem.at[2]), pltpu.make_async_copy(su, rb.at[1], lsem.at[3])]
    shared_load += [pltpu.make_async_copy(sd.at[:, i * part:(i + 1) * part], hb.at[i], lsem.at[4 + i]) for i in range(experts)]
    last = experts - 1
    start(shared_load)
    for e in range(experts):
        start(loads13[e])
    start(loads2)
    blk = 512

    def block(i):
        return pl.ds(pl.multiple_of(i * blk, blk), blk)

    def wait_recv(copies):
        for c in copies:
            c.wait_recv()

    def pick(p, a, b):
        mb[p] = jnp.zeros(mb.shape[1:], BF16)
        for s, slot in enumerate((a, b)):
            info = meta[slot]
            row = lax.broadcasted_iota(jnp.int32, (experts * slots, tok), 0)
            key = (row + me * (experts * slots)).astype(F32)
            hit = jnp.zeros((experts * slots, tok), F32)
            gate = jnp.zeros((experts * slots, tok), F32)
            for j in range(top_k):
                eq = key == info[j:j + 1, :]
                hit = jnp.where(eq, 1.0, hit)
                gate = jnp.where(eq, info[16 + j:17 + j, :], gate)
            hit = hit.astype(BF16)
            gate = jnp.broadcast_to(jnp.sum(gate, axis=1, keepdims=True), (experts * slots, tok))
            for e in range(experts):
                dst = slice(e * pairw + s * slots, e * pairw + (s + 1) * slots)
                mb[p, dst, s * tok:(s + 1) * tok] = hit[e * slots:(e + 1) * slots]
                gb[p, dst, :] = gate[e * slots:(e + 1) * slots]

    def gather(src, p, a, b, gated):
        col = 256
        at = (p % 2) * pairw
        for i in range(dim // col):
            cols = slice(i * col, (i + 1) * col)
            r = dot(mb[p], jnp.concatenate([src[a, :, cols], src[b, :, cols]], axis=0))
            if gated:
                r = r * jnp.concatenate([gb[p]] * (col // tok), axis=1)
            r = r.astype(BF16)
            for e in range(experts):
                rows_b[e, at:at + pairw, cols] = r[e * pairw:(e + 1) * pairw]

    def kept(out, g, n):
        return pltpu.make_async_copy(rows_b, out.at[:, g * half:(g + 1) * half], osem.at[n])

    def expert_loop(body, events):
        @pl.loop(0, experts)
        def _(e):
            for at, event in events:
                pl.when(e == at)(event)
            body(e)

    def acts(g):
        def body(e):
            db[e, g * half:(g + 1) * half, :ff] = dot(rows_b[e], w1b[e]).astype(BF16)
            db[e, g * half:(g + 1) * half, ff:] = dot(rows_b[e], w3b[e]).astype(BF16)
        return body

    def grads(g, events):
        rows = slice(g * half, (g + 1) * half)

        def hidden_grads(e):
            grad_hidden = dot(w2b[e], rows_b[e], NT).T
            hidden, grad_gate, grad_up = swiglu_parts(db[e, rows, :ff], db[e, rows, ff:], grad_hidden)
            db[e, rows, :ff] = grad_gate
            db[e, rows, ff:] = grad_up
            hb[e, :, rows] = hidden.T

        def input_grads(e):
            for i in range(dim // blk):
                part = slice(i * blk, (i + 1) * blk)
                r = (dot(w1b[e, part, :], db[e, rows, :ff], NT) + dot(w3b[e, part, :], db[e, rows, ff:], NT)).astype(BF16)
                for p in range(2):
                    rb[p, part, e * pairw:(e + 1) * pairw] = r[:, p * pairw:(p + 1) * pairw]

        hidden_grads(0)
        for e in range(experts):
            for at, event in events:
                if at == e:
                    event()
            if e + 1 < experts:
                hidden_grads(e + 1)
            input_grads(e)

    def combine(p):
        q = p % 2

        for i in range(dim // blk):
            part = slice(i * blk, (i + 1) * blk)
            s = dot(rb[q, part, :], mb[p])
            pb[2 * q, part, :] = s[:, :tok]
            pb[2 * q + 1, part, :] = s[:, tok:]

    def side(frm, to_slot):
        return remote(pb.at[frm], pr.at[to_slot], psend.at[to_slot], precv.at[to_slot], partner)

    def add(to_slot, terms):
        @pl.loop(0, dim // blk)
        def _(i):
            v = pr[to_slot, block(i), :]
            for t in terms:
                v = v + t[block(i), :]
            pr[to_slot, block(i), :] = v

    wait_recv(metas[:1])
    pick(0, 0, 1)

    for c in shared_load:
        c.wait()
    act_gate = dot(xg[0], rb[0])
    act_up = dot(xg[0], rb[1])
    grad_hidden = dot(hb[0], yg[0, :, :part], NT)
    for i in range(1, experts):
        grad_hidden += dot(hb[i], yg[0, :, i * part:(i + 1) * part], NT)
    hidden, grad_gate, grad_up = swiglu_parts(act_gate.astype(BF16), act_up.astype(BF16), grad_hidden.T)
    dsb[:, :ff] = grad_gate
    dsb[:, ff:] = grad_up
    hsb[...] = hidden.T
    shared_out = [pltpu.make_async_copy(dsb, ds_out, osem.at[0]), pltpu.make_async_copy(hsb, hs_out, osem.at[1])]
    start(shared_out)
    for i in range(dim // blk):
        rows = slice(i * blk, (i + 1) * blk)
        shr[rows, :] = dot(rb[0, rows, :], dsb[:, :ff], NT) + dot(rb[1, rows, :], dsb[:, ff:], NT)

    xs[1].wait_recv()
    gather(xg, 0, 0, 1, False)
    wait_recv(metas[1:])
    pick(1, 2, 3)

    xs[2].wait_recv()
    xs[4].start()
    xs[3].start()
    pick(2, 4, 5)
    pick(3, 6, 7)
    xs[3].wait_recv()
    xs[6].start()
    ys[6].start()
    gather(xg, 1, 2, 3, False)
    keep_x0 = kept(x_out, 0, 2)
    keep_x0.start()

    def have_weights(e):
        def event():
            for c in loads13[e]:
                c.wait()
        return event

    def near_on():
        ys[2].wait_recv()
        ys[4].start()
        ys[3].start()

    expert_loop(acts(0), [(e, have_weights(e)) for e in range(experts)] + [(last, near_on)])
    keep_x0.wait()
    ys[1].wait_recv()
    gather(yg, 0, 0, 1, True)
    ys[3].wait_recv()
    gather(yg, 1, 2, 3, True)
    keep_z0 = kept(z_out, 0, 4)
    keep_z0.start()
    for c in loads2:
        c.wait()

    def x_sides():
        xs[4].wait_recv()
        xs[5].start()
        xs[6].wait_recv()
        xs[7].start()

    grads(0, [(last, x_sides)])
    combine(0)
    to_own = side(1, 0)
    to_own.start()
    combine(1)
    to_near = side(3, 1)
    to_near.start()

    keep_z0.wait()
    xs[5].wait_recv()
    gather(xg, 2, 4, 5, False)
    xs[7].wait_recv()
    gather(xg, 3, 6, 7, False)
    keep_x1 = kept(x_out, 1, 3)
    keep_x1.start()
    own_copy = pltpu.make_async_copy(pr.at[0], own_out, osem.at[8])
    ret_near = remote(pr.at[1], near_out, rsem.at[0], rsem.at[1], prv)

    def sum_near():
        to_near.wait()
        add(1, [pb.at[2]])
        ret_near.start()
        to_own.wait()
        add(0, [pb.at[0], shr])
        own_copy.start()

    expert_loop(acts(1), [(1, sum_near)])
    ys[4].wait_recv()
    ys[5].start()
    ys[6].wait_recv()
    ys[7].start()
    keep_x1.wait()
    ys[5].wait_recv()
    gather(yg, 2, 4, 5, True)
    ys[7].wait_recv()
    gather(yg, 3, 6, 7, True)
    keep_z1 = kept(z_out, 1, 5)
    keep_z1.start()
    grads(1, [])
    keep_d = [pltpu.make_async_copy(db, d_out, osem.at[6]), pltpu.make_async_copy(hb, h_out, osem.at[7])]
    start(keep_d)
    combine(2)
    to_far = side(1, 2)
    to_far.start()
    combine(3)
    to_back = side(3, 3)
    to_back.start()
    to_far.wait()
    add(2, [pb.at[0]])
    far_copy = pltpu.make_async_copy(pr.at[2], far_out, osem.at[9])
    far_copy.start()
    to_back.wait()
    add(3, [pb.at[2]])
    back_copy = pltpu.make_async_copy(pr.at[3], back_out, osem.at[10])
    back_copy.start()
    ret_near.wait()
    for c in shared_out + [keep_z1] + keep_d + [own_copy, far_copy, back_copy]:
        c.wait()
    for c in list(xs.values()) + list(ys.values()) + metas:
        c.wait_send()


def layer(chips, x, dy, ids, pos, gates, weights, shared, slots):
    experts, dim, ff = weights[0].shape
    top_k, tok = ids.shape
    pairw = 2 * slots
    rows = chips * pairw
    half = 2 * pairw
    dma = pltpu.SemaphoreType.DMA
    sds = jax.ShapeDtypeStruct
    hbm = pl.BlockSpec(memory_space=pltpu.HBM)
    return pl.pallas_call(
        functools.partial(layer_kernel, chips, top_k, slots),
        name='layer',
        out_shape=(sds((experts, rows, dim), BF16), sds((experts, rows, dim), BF16), sds((experts, rows, 2 * ff), BF16), sds((experts, ff, rows), BF16),
                   sds((tok, 2 * ff), BF16), sds((ff, tok), BF16), sds((dim, tok), F32), sds((dim, tok), F32), sds((dim, tok), F32), sds((dim, tok), F32)),
        in_specs=[hbm] * 2 + [VMEM] * 3 + [hbm] * 6,
        out_specs=(hbm,) * 10,
        scratch_shapes=[
            pltpu.VMEM((8, tok, dim), BF16), pltpu.VMEM((8, tok, dim), BF16), pltpu.VMEM((8, 32, tok), F32),
            pltpu.VMEM((experts, dim, ff), BF16), pltpu.VMEM((experts, dim, ff), BF16), pltpu.VMEM((experts, ff, dim), BF16),
            pltpu.VMEM((experts, half, dim), BF16),
            pltpu.VMEM((2, dim, experts * pairw), BF16),
            pltpu.VMEM((experts, rows, 2 * ff), BF16), pltpu.VMEM((experts, ff, rows), BF16),
            pltpu.VMEM((tok, 2 * ff), BF16), pltpu.VMEM((ff, tok), BF16), pltpu.VMEM((dim, tok), F32),
            pltpu.VMEM((4, dim, tok), F32), pltpu.VMEM((4, dim, tok), F32),
            pltpu.VMEM((4, experts * pairw, 2 * tok), BF16), pltpu.VMEM((4, experts * pairw, tok), F32),
            dma((4 + experts,)), dma((3, experts)), dma((12,)), dma((8,)), dma((8,)), dma((8,)), dma((8,)), dma((8,)), dma((8,)), dma((4,)), dma((4,)), dma((2,)),
        ],
        compiler_params=pltpu.CompilerParams(vmem_limit_bytes=67043328, collective_id=0, has_side_effects=True),
        cost_estimate=pl.CostEstimate(flops=10 * experts * rows * dim * ff, bytes_accessed=3 * experts * dim * ff * 2, transcendentals=experts * rows * ff),
    )(x, dy, ids, pos, gates, *weights, *shared)


def grad_kernel(first, count, shared, prior, *refs):
    n_in = 8
    ins, refs = refs[:n_in], refs[n_in + prior:]
    n_out = 6
    outs, (xb, zb, db, hb, sx, sz, sd, sh, g1b, g3b, g2b, dsem, ssem, osem) = refs[:n_out], refs[n_out:]
    x, z, d, h = ins[:4]
    ff = h.shape[1]
    dim = x.shape[2]
    blk = g1b.shape[1]
    blocks = dim // blk
    fblk = ff // blocks

    def cols(i):
        return pl.ds(pl.multiple_of(i * blk, blk), blk)

    def inputs(n):
        b = n % 2
        return [pltpu.make_async_copy(a.at[first + n], v.at[b], dsem.at[k, b]) for k, (a, v) in enumerate(((d, db), (x, xb), (h, hb), (z, zb)))]

    def fetch(n):
        for c in inputs(n):
            c.start()

    def rows(i):
        return pl.ds(pl.multiple_of(i * fblk, fblk), fblk)

    def stores(dst, e, i):
        return [pltpu.make_async_copy(g1b.at[i], dst[0].at[e, cols(i), :], osem.at[0, i]),
                pltpu.make_async_copy(g3b.at[i], dst[1].at[e, cols(i), :], osem.at[1, i]),
                pltpu.make_async_copy(g2b.at[i], dst[2].at[e, rows(i), :], osem.at[2, i])]

    def item(dst, e, span, xv, zv, dv, hv, busy):
        @pl.loop(*span)
        def _(i):
            @pl.when((i >= busy[0]) & (i < busy[1]))
            def _():
                for c in stores(dst, e, i):
                    c.wait()
            x_t = xv[:, cols(i)].T
            g1b[i] = dot(x_t, dv[:, :ff])
            g3b[i] = dot(x_t, dv[:, ff:])
            g2b[i] = dot(hv[rows(i), :], zv[...])
            for c in stores(dst, e, i):
                c.start()

    own = [pltpu.make_async_copy(a, b, ssem.at[i]) for i, (a, b) in enumerate(zip(ins[4:], (sx, sz, sd, sh)))]
    for c in own:
        c.start()
    fetch(0)
    for c in own:
        c.wait()
    item(outs[3:], 0, shared, sx, sz, sd, sh, (0, 0))
    for n in range(count):
        if n + 1 < count:
            fetch(n + 1)
        for c in inputs(n):
            c.wait()
        b = n % 2
        item(outs[:3], first + n, (0, blocks), xb.at[b], zb.at[b], db.at[b], hb.at[b], (0, blocks) if n else shared)

    @pl.loop(0, blocks)
    def _(i):
        for c in stores(outs[:3], first, i):
            c.wait()


def weight_grads(x, z, d, h, shared, first, count, span, prior=()):
    experts, rows, dim = x.shape
    ff = h.shape[1]
    tok = shared[0].shape[0]
    blk = 1024
    blocks = dim // blk
    span = tuple(blocks * n // 4 for n in span)
    hbm = pl.BlockSpec(memory_space=pltpu.HBM)
    sds = jax.ShapeDtypeStruct
    dma = pltpu.SemaphoreType.DMA
    out_shape = (sds((experts, dim, ff), F32), sds((experts, dim, ff), F32), sds((experts, ff, dim), F32),
                 sds((1, dim, ff), F32), sds((1, dim, ff), F32), sds((1, ff, dim), F32))
    return pl.pallas_call(
        functools.partial(grad_kernel, first, count, span, len(prior)),
        name='weight_grads',
        in_specs=[hbm] * (8 + len(prior)),
        out_specs=(hbm,) * 6,
        out_shape=out_shape,
        input_output_aliases={8 + i: i for i in range(len(prior))},
        scratch_shapes=[
            pltpu.VMEM((2, rows, dim), BF16), pltpu.VMEM((2, rows, dim), BF16), pltpu.VMEM((2, rows, 2 * ff), BF16), pltpu.VMEM((2, ff, rows), BF16),
            pltpu.VMEM((tok, dim), BF16), pltpu.VMEM((tok, dim), BF16), pltpu.VMEM((tok, 2 * ff), BF16), pltpu.VMEM((ff, tok), BF16),
            pltpu.VMEM((blocks, blk, ff), F32), pltpu.VMEM((blocks, blk, ff), F32), pltpu.VMEM((blocks, ff // blocks, dim), F32),
            dma((4, 2)), dma((4,)), dma((3, blocks)),
        ],
        compiler_params=pltpu.CompilerParams(vmem_limit_bytes=60 * 2**20),
        cost_estimate=pl.CostEstimate(flops=6 * count * rows * dim * ff, bytes_accessed=count * dim * (rows * 4 + ff * 12), transcendentals=0),
    )(x, z, d, h, *shared, *prior)


def final_kernel(a, b, c, out):
    out[...] = (a[...] + b[...] + c[...]).T.astype(BF16)


def final_sum(*terms):
    dim, tok = terms[0].shape
    blk = 1024
    return pl.pallas_call(
        final_kernel,
        name='final_sum',
        grid=(dim // blk,),
        in_specs=[pl.BlockSpec((blk, tok), lambda i: (i, 0))] * 3,
        out_specs=pl.BlockSpec((tok, blk), lambda i: (0, i)),
        out_shape=jax.ShapeDtypeStruct((tok, dim), BF16),
        compiler_params=pltpu.CompilerParams(vmem_limit_bytes=12 * 2**20),
        cost_estimate=pl.CostEstimate(flops=5 * dim * tok, bytes_accessed=dim * tok * 14, transcendentals=0),
    )(*terms)


def solution(mesh):
    group = mesh.shape['ep']
    cores = 2
    chips = group // cores
    token_spec = P(('dp', 'ep'), None)
    expert_spec = P('ep', None, None)
    whole_spec = P(None, None)
    grad_spec = P(('dp', 'ep'), None, None)

    assert chips == 4

    def shift(step):
        return [(c * cores + k, ((c + (step if k == 0 else -step)) % chips) * cores + k) for c in range(chips) for k in range(cores)]

    def local_backward(x_tokens, dy_tokens, expert_ids, gate_vals, slot_pos, w_gate, w_up, w_down, shared_gate, shared_up, shared_down):
        tok, top_k = expert_ids.shape
        num_experts = w_gate.shape[0] * group
        ff = w_gate.shape[2]
        capacity = (3 * tok * top_k + 2 * num_experts - 1) // (2 * num_experts)
        slots = pl.cdiv(capacity, 64) * 64
        x, z, d, h, ds, hs, own_sum, ret_near, far_sum, back_sum = layer(chips, x_tokens, dy_tokens, expert_ids.T, slot_pos.T, gate_vals.T, (w_gate, w_up, w_down), (shared_gate, shared_up, shared_down), slots)
        via = lax.ppermute(far_sum, 'ep', shift(1))
        half_experts = w_gate.shape[0] // 2
        shared = (x_tokens, dy_tokens, ds, hs)
        first = weight_grads(x, z, d, h, shared, 0, half_experts, (0, 2))
        via, first = lax.optimization_barrier((via, first))
        ret_back = lax.ppermute(back_sum + via, 'ep', shift(1))
        g1, g3, g2, gsg, gsu, gsd = weight_grads(x, z, d, h, shared, half_experts, w_gate.shape[0] - half_experts, (2, 4), tuple(first))
        grad_x = final_sum(own_sum, ret_near, ret_back)
        return grad_x, g1, g3, g2, gsg, gsu, gsd

    return jax.shard_map(local_backward, mesh=mesh, in_specs=(token_spec, token_spec, token_spec, token_spec, token_spec, expert_spec, expert_spec, expert_spec, whole_spec, whole_spec, whole_spec), out_specs=(token_spec, grad_spec, grad_spec, grad_spec, grad_spec, grad_spec, grad_spec), check_vma=False)
```
